8 devices in a mesh: batch: 1 (over z), dap: 8 (over y, x, core).
Axes of the slice: x: 2, y: 2, z: 1, core: 2. Of those that a mesh axis runs over, the one named last changes fastest.
Arguments:
- z_pair: bfloat16 [512, 512, 128], P(('batch', 'dap'))
- pair_mask: int32 [512, 512], P(('batch', 'dap'))
- dz_out: bfloat16 [512, 512, 128], P(('batch', 'dap'))
- ln_in_scale: bfloat16 [128], replicated
- ln_in_offset: bfloat16 [128], replicated
- w_in: bfloat16 [128, 512], replicated
- b_in: bfloat16 [512], replicated
- ln_out_scale: bfloat16 [128], replicated
- ln_out_offset: bfloat16 [128], replicated
- w_out: bfloat16 [128, 128], replicated
- b_out: bfloat16 [128], replicated
- w_gate: bfloat16 [128, 128], replicated
- b_gate: bfloat16 [128], replicated
Outputs:
- output 1: bfloat16 [512, 512, 128], P(('batch', 'dap'))
- output 2: bfloat16 [128], P('batch')
- output 3: bfloat16 [128], P('batch')
- output 4: bfloat16 [128, 512], P('batch')
- output 5: bfloat16 [512], P('batch')
- output 6: bfloat16 [128], P('batch')
- output 7: bfloat16 [128], P('batch')
- output 8: bfloat16 [128, 128], P('batch')
- output 9: bfloat16 [128], P('batch')
- output 10: bfloat16 [128, 128], P('batch')
- output 11: bfloat16 [128], P('batch')
All inputs are finite; a program needn't handle non-finite values.
Results may differ from the reference program's by a relative error of at most 0.0125153.
Values are sent between devices in bfloat16 or wider.
A program may use at most 1 GiB of HBM per device.

```python
import functools
import jax
import jax.numpy as jnp
from jax import lax

N = 512
CZ = 128
CH = 128
LN_EPS = 1e-5


@jax.custom_vjp
def dense_map(x_act, w_mat):
    return jnp.einsum('...k,km->...m', x_act.astype(jnp.float32), w_mat.astype(jnp.float32))


def dense_fwd(x_act, w_mat):
    return dense_map(x_act, w_mat), (x_act, w_mat)


def dense_bwd(saved_res, grad_out):
    x_act, w_mat = saved_res
    grad_b16 = grad_out.astype(jnp.bfloat16).astype(jnp.float32)
    grad_x = jnp.einsum('...m,km->...k', grad_b16, w_mat.astype(jnp.float32)).astype(jnp.bfloat16)
    grad_w = jnp.einsum('...k,...m->km', x_act.astype(jnp.float32), grad_b16).astype(jnp.bfloat16)
    return grad_x, grad_w


dense_map.defvjp(dense_fwd, dense_bwd)


@jax.custom_vjp
def triangle_map(act_a, act_b):
    return jnp.einsum('ikc,jkc->ijc', act_a.astype(jnp.float32), act_b.astype(jnp.float32))


def triangle_fwd(act_a, act_b):
    return triangle_map(act_a, act_b), (act_a, act_b)


def triangle_bwd(saved_res, grad_out):
    act_a, act_b = saved_res
    grad_b16 = grad_out.astype(jnp.bfloat16).astype(jnp.float32)
    grad_a = jnp.einsum('ijc,jkc->ikc', grad_b16, act_b.astype(jnp.float32)).astype(jnp.bfloat16)
    grad_bb = jnp.einsum('ijc,ikc->jkc', grad_b16, act_a.astype(jnp.float32)).astype(jnp.bfloat16)
    return grad_a, grad_bb


triangle_map.defvjp(triangle_fwd, triangle_bwd)


def layer_norm(x_val, ln_scale, ln_offset):
    mean_val = jnp.mean(x_val, axis=-1, keepdims=True)
    centered = x_val - mean_val
    var_val = jnp.mean(centered * centered, axis=-1, keepdims=True)
    return centered * lax.rsqrt(var_val + LN_EPS) * ln_scale.astype(jnp.float32) + ln_offset.astype(jnp.float32)


def outgoing_layer(z_pair, ln_in_scale, ln_in_offset, w_in, b_in, ln_out_scale, ln_out_offset, w_out, b_out, w_gate, b_gate, pair_mask):
    z_f = z_pair.astype(jnp.float32)
    z_norm = layer_norm(z_f, ln_in_scale, ln_in_offset).astype(jnp.bfloat16)
    w_cat = jnp.concatenate([w_in, w_gate], axis=1)
    b_cat = jnp.concatenate([b_in, b_gate]).astype(jnp.float32)
    proj_all = dense_map(z_norm, w_cat) + b_cat
    mask_f = pair_mask.astype(jnp.float32)[..., None]
    proj_a = proj_all[..., :CH]
    proj_b = proj_all[..., CH:2 * CH]
    sig_a = jax.nn.sigmoid(proj_all[..., 2 * CH:3 * CH])
    sig_b = jax.nn.sigmoid(proj_all[..., 3 * CH:4 * CH])
    sig_g = jax.nn.sigmoid(proj_all[..., 4 * CH:])
    act_a = (mask_f * sig_a * proj_a).astype(jnp.bfloat16)
    act_b = (mask_f * sig_b * proj_b).astype(jnp.bfloat16)
    tri_out = triangle_map(act_a, act_b)
    o_norm = layer_norm(tri_out, ln_out_scale, ln_out_offset).astype(jnp.bfloat16)
    update = (dense_map(o_norm, w_out) + b_out.astype(jnp.float32)).astype(jnp.bfloat16)
    return (z_f + sig_g * update.astype(jnp.float32)).astype(jnp.bfloat16)


def setup_inputs(seed: int = 0, part: int = 0) -> dict:
    part_key = jax.random.fold_in(jax.random.key(seed), part)
    k_z, k_dy, k_res, k_pair = jax.random.split(part_key, 4)
    w_keys = jax.random.split(jax.random.key(seed + 1), 12)
    res_keep = (jax.random.randint(k_res, (N,), 0, 8) != 0).astype(jnp.int32)
    pair_keep = (jax.random.randint(k_pair, (N, N), 0, 16) != 0).astype(jnp.int32)
    pair_mask = res_keep[:, None] * res_keep[None, :] * pair_keep
    return {
        'z_pair': jax.random.normal(k_z, (N, N, CZ), jnp.float32).astype(jnp.bfloat16),
        'pair_mask': pair_mask,
        'dz_out': jax.random.normal(k_dy, (N, N, CZ), jnp.float32).astype(jnp.bfloat16),
        'ln_in_scale': (1.0 + 0.3 * jax.random.normal(w_keys[0], (CZ,), jnp.float32)).astype(jnp.bfloat16),
        'ln_in_offset': (0.3 * jax.random.normal(w_keys[1], (CZ,), jnp.float32)).astype(jnp.bfloat16),
        'w_in': (jax.random.normal(w_keys[2], (CZ, 4 * CH), jnp.float32) * CZ ** -0.5).astype(jnp.bfloat16),
        'b_in': (0.5 * jax.random.normal(w_keys[3], (4 * CH,), jnp.float32)).astype(jnp.bfloat16),
        'ln_out_scale': (1.0 + 0.3 * jax.random.normal(w_keys[4], (CH,), jnp.float32)).astype(jnp.bfloat16),
        'ln_out_offset': (0.3 * jax.random.normal(w_keys[5], (CH,), jnp.float32)).astype(jnp.bfloat16),
        'w_out': (jax.random.normal(w_keys[6], (CH, CZ), jnp.float32) * CH ** -0.5).astype(jnp.bfloat16),
        'b_out': (0.5 * jax.random.normal(w_keys[7], (CZ,), jnp.float32)).astype(jnp.bfloat16),
        'w_gate': (jax.random.normal(w_keys[8], (CZ, CZ), jnp.float32) * CZ ** -0.5).astype(jnp.bfloat16),
        'b_gate': (0.5 * jax.random.normal(w_keys[9], (CZ,), jnp.float32)).astype(jnp.bfloat16),
    }


def reference(z_pair, pair_mask, dz_out, ln_in_scale, ln_in_offset, w_in, b_in, ln_out_scale, ln_out_offset, w_out, b_out, w_gate, b_gate):
    layer_fn = functools.partial(outgoing_layer, pair_mask=pair_mask)
    z_next, vjp_fn = jax.vjp(layer_fn, z_pair, ln_in_scale, ln_in_offset, w_in, b_in, ln_out_scale, ln_out_offset, w_out, b_out, w_gate, b_gate)
    d_z, d_in_scale, d_in_offset, d_w_in, d_b_in, d_out_scale, d_out_offset, d_w_out, d_b_out, d_w_gate, d_b_gate = vjp_fn(dz_out)
    return (d_z, d_in_scale, d_in_offset, d_w_in, d_b_in, d_out_scale, d_out_offset, d_w_out, d_b_out, d_w_gate, d_b_gate)
```

```python
import jax
import jax.numpy as jnp
from jax import lax
from jax.experimental import pallas as pl
from jax.experimental.pallas import tpu as pltpu
from jax.sharding import PartitionSpec as P

LN_EPS = 1e-5
N = 512
C = 128
NR = 64
NB = 16
NQ = NR // NB
HALF = NR // 2
HOPS = ((0, 0), (2, 4), (6, 6), (4, 2))
SB = NB + 8
SO = NR + 8
F32 = jnp.float32
BF16 = jnp.bfloat16
VMEM_LIMIT = 60 * 1024 * 1024


def sds(shape, dtype):
    return jax.ShapeDtypeStruct(shape, dtype)


def full_spec(shape):
    return pl.BlockSpec(shape, lambda *ids: (0,) * len(shape))


def sigmoid(x_val):
    return 1.0 / (1.0 + jnp.exp(-x_val))


def nt_dot(lhs, rhs):
    return lax.dot_general(lhs, rhs, (((1,), (1,)), ((), ())), preferred_element_type=F32)


def nn_dot(lhs, rhs):
    return lax.dot_general(lhs, rhs, (((1,), (0,)), ((), ())), preferred_element_type=F32)


def ones_rows(width):
    return jnp.where(lax.broadcasted_iota(jnp.int32, (16, width), 0) == 0, 1.0, 0.0).astype(BF16)


def norm_rows(x_val):
    mean_val = jnp.mean(x_val, axis=0, keepdims=True)
    centered = x_val - mean_val
    inv_std = lax.rsqrt(jnp.mean(centered * centered, axis=0, keepdims=True) + LN_EPS)
    return centered * inv_std, inv_std


def put_row(scr, row, pitch, val):
    for lane in range(val.shape[1] // 128):
        scr[lane, pl.ds(row, C, stride=pitch), :] = val[:, 128 * lane:128 * (lane + 1)]


def get_row(scr, row, pitch):
    return jnp.concatenate([scr[lane, pl.ds(row, C, stride=pitch), :] for lane in range(scr.shape[0])], axis=1)


def flush_rows(scr, out_ref, pitch):
    rows = out_ref.shape[1]

    def body(ch, carry):
        base = pl.multiple_of(ch * pitch, 8)
        for lane in range(scr.shape[0]):
            out_ref[ch, :, 128 * lane:128 * (lane + 1)] = scr[lane, pl.ds(base, rows), :].astype(BF16)
        return carry

    lax.fori_loop(0, C, body, 0, unroll=8)


def pair_row(ref, row, ids_ref):
    return jnp.concatenate([ref[row, pl.ds(pl.multiple_of(ids_ref[p], HALF), HALF), :] for p in range(16)], axis=0)


def normed_row(z_row, scale, offset):
    z_t = z_row.T.astype(F32)
    x_hat, inv_std = norm_rows(z_t)
    z_norm = (x_hat * scale + offset).astype(BF16)
    return x_hat, inv_std, z_norm


def pass_ids(ids_ref, tok_ref):
    for p in range(17):
        tok_ref[p] = ids_ref[p]


TOKEN = sds((17,), jnp.int32)
TOKEN_SPEC = pl.BlockSpec(memory_space=pltpu.SMEM)


def load_mask(m_ref, m_scr, ids_ref):
    m_scr[...] = pair_row(m_ref, 0, ids_ref).astype(F32).T


def gated_kernel(ids_ref, z_ref, m_ref, w_ref, scale_ref, offset_ref, a_ref, b_ref, tok_ref, a_scr, b_scr, m_scr):
    pass_ids(ids_ref, tok_ref)
    load_mask(m_ref, m_scr, ids_ref)
    first = pl.program_id(0) * NB

    def body(row, carry):
        _, _, z_norm = normed_row(pair_row(z_ref, row, ids_ref), scale_ref[...], offset_ref[...])
        aug = jnp.concatenate([z_norm, ones_rows(N)], axis=0)
        mask_f = m_scr[pl.ds(first + row, 1), :]
        for side, scr in ((0, a_scr), (1, b_scr)):
            proj = nn_dot(w_ref[side * C:(side + 1) * C], aug)
            sig = sigmoid(nn_dot(w_ref[(2 + side) * C:(3 + side) * C], aug))
            put_row(scr, row, SB, mask_f * sig * proj)
        return carry

    lax.fori_loop(0, NB, body, 0, unroll=4)
    flush_rows(a_scr, a_ref, SB)
    flush_rows(b_scr, b_ref, SB)


def gated_call(ids, piece, w_t, scale, offset):
    out_spec = pl.BlockSpec((C, NB, N), lambda r, ids: (0, r, 0))
    return pl.pallas_call(
        gated_kernel,
        grid_spec=pltpu.PrefetchScalarGridSpec(
            num_scalar_prefetch=1,
            grid=(HALF // NB,),
            in_specs=[
                pl.BlockSpec((NB, N, C), lambda r, ids: (r, 0, 0)),
                pl.BlockSpec((1, N, C), lambda r, ids: (HALF, 0, 0)),
                full_spec((4 * C, C + 16)), full_spec((C, N)), full_spec((C, N)),
            ],
            out_specs=[out_spec, out_spec, TOKEN_SPEC],
            scratch_shapes=[pltpu.VMEM((4, C * SB, 128), F32)] * 2 + [pltpu.VMEM((C, N), F32)],
        ),
        out_shape=[sds((C, HALF, N), BF16)] * 2 + [TOKEN],
        compiler_params=pltpu.CompilerParams(vmem_limit_bytes=VMEM_LIMIT),
        cost_estimate=pl.CostEstimate(flops=2 * 32 * 512 * 144 * 512, bytes_accessed=12 << 20, transcendentals=1 << 22),
        name="gated_rows",
    )(ids, piece, piece, w_t, scale, offset)


def lanes(val):
    return val[:, :128] + val[:, 128:256] + (val[:, 256:384] + val[:, 384:])


def own_kernel(ids_ref, z_ref, dy_ref, m_ref, w_ref, scale_ref, offset_ref, w_out_ref,
               a_ref, b_ref, dup_ref, don_ref, g1_ref, dbout_ref, dooff_ref, tok_ref, a_scr, b_scr, m_scr):
    pass_ids(ids_ref, tok_ref)

    @pl.when(pl.program_id(0) == 0)
    def _():
        dbout_ref[...] = jnp.zeros_like(dbout_ref)
        dooff_ref[...] = jnp.zeros_like(dooff_ref)

    load_mask(m_ref, m_scr, ids_ref)
    first = pl.program_id(0) % 2 * NB

    def body(row, carry):
        _, _, z_norm = normed_row(pair_row(z_ref, row, ids_ref), scale_ref[...], offset_ref[...])
        aug = jnp.concatenate([z_norm, ones_rows(N)], axis=0)
        mask_f = m_scr[pl.ds(first + row, 1), :]
        for side, scr in ((0, a_scr), (1, b_scr)):
            proj = nn_dot(w_ref[side * C:(side + 1) * C], aug)
            sig = sigmoid(nn_dot(w_ref[(2 + side) * C:(3 + side) * C], aug))
            put_row(scr, row, SB, mask_f * sig * proj)
        sig_g = sigmoid(nn_dot(w_ref[4 * C:5 * C], aug))
        dy_t = pair_row(dy_ref, row, ids_ref).T.astype(F32)
        d_upd = sig_g * dy_t
        g1_ref[row] = d_upd * (1.0 - sig_g)
        d_upd16 = d_upd.astype(BF16)
        dup_ref[row] = d_upd16
        d_onorm = nn_dot(w_out_ref[...], d_upd16).astype(BF16)
        don_ref[row] = d_onorm
        dbout_ref[...] += lanes(d_upd16.astype(F32))
        dooff_ref[...] += lanes(d_onorm.astype(F32))
        return carry

    lax.fori_loop(0, NB, body, 0, unroll=2)
    flush_rows(a_scr, a_ref, SB)
    flush_rows(b_scr, b_ref, SB)


def own_call(ids, z_loc, dy_loc, m_loc, w_t, scale, offset, w_out):
    row_spec = pl.BlockSpec((NB, N, C), lambda r, ids: (r, 0, 0))
    t_spec = pl.BlockSpec((NB, C, N), lambda r, ids: (r, 0, 0))
    act_spec = pl.BlockSpec((C, NB, N), lambda r, ids: (0, r, 0))
    return pl.pallas_call(
        own_kernel,
        grid_spec=pltpu.PrefetchScalarGridSpec(
            num_scalar_prefetch=1,
            grid=(NQ,),
            in_specs=[row_spec, row_spec, pl.BlockSpec((1, N, C), lambda r, ids: (r // 2, 0, 0)),
                      full_spec((5 * C, C + 16)), full_spec((C, N)), full_spec((C, N)), full_spec((C, C))],
            out_specs=[act_spec, act_spec, t_spec, t_spec, t_spec, full_spec((C, 128)), full_spec((C, 128)), TOKEN_SPEC],
            scratch_shapes=[pltpu.VMEM((4, C * SB, 128), F32)] * 2 + [pltpu.VMEM((C, N), F32)],
        ),
        out_shape=[sds((C, NR, N), BF16), sds((C, NR, N), BF16), sds((NR, C, N), BF16), sds((NR, C, N), BF16), sds((NR, C, N), F32), sds((C, 128), F32), sds((C, 128), F32), TOKEN],
        compiler_params=pltpu.CompilerParams(vmem_limit_bytes=VMEM_LIMIT),
        cost_estimate=pl.CostEstimate(flops=2 * 64 * 512 * 144 * 512, bytes_accessed=64 << 20, transcendentals=1 << 23),
        name="own_rows",
    )(ids, z_loc, dy_loc, m_loc, w_t, scale, offset, w_out)


CB = 16


def out_kernel(ids_ref, a_ref, b_own0, b_own1, b_par0, b_par1, don_ref, dup_ref, g1_ref, w_out_ref, scale_ref, offset_ref,
               do_ref, dg_ref, same0, same1, cross0, cross1, dwout_ref, dosc_ref, dbg_ref, tok_ref, o_scr):
    pass_ids(ids_ref, tok_ref)
    step = pl.program_id(0)
    first_core = ids_ref[16] == 0

    def prod(ch, carry):
        base = pl.multiple_of((step * CB + ch) * SO, 8)
        own = jnp.concatenate([b_own0[ch], b_own1[ch]], axis=0)
        par = jnp.concatenate([b_par0[ch], b_par1[ch]], axis=0)
        val = nt_dot(a_ref[ch], jnp.concatenate([own, par], axis=0))
        o_scr[0, pl.ds(base, NR), :] = jnp.where(first_core, val, pltpu.roll(val, 64, 1))
        return carry

    lax.fori_loop(0, CB, prod, 0, unroll=8)

    @pl.when(step == C // CB - 1)
    def _():
        dwout_ref[...] = jnp.zeros_like(dwout_ref)
        dosc_ref[...] = jnp.zeros_like(dosc_ref)
        dbg_ref[...] = jnp.zeros_like(dbg_ref)

        def chain(row, carry):
            o_hat, inv_std = norm_rows(get_row(o_scr, row, SO))
            o_norm = (o_hat * scale_ref[...] + offset_ref[...]).astype(BF16)
            aug = jnp.concatenate([o_norm, ones_rows(128)], axis=0)
            upd = nn_dot(w_out_ref[...], aug).astype(BF16).astype(F32)
            d_gate = g1_ref[row] * upd
            dbg_ref[...] += d_gate
            dg_ref[row] = d_gate.astype(BF16)
            d_onorm = don_ref[row].astype(F32)
            dosc_ref[...] += d_onorm * o_hat
            grad_hat = d_onorm * scale_ref[...]
            mean_grad = jnp.mean(grad_hat, axis=0, keepdims=True)
            mean_proj = jnp.mean(grad_hat * o_hat, axis=0, keepdims=True)
            put_row(o_scr, row, SO, inv_std * (grad_hat - mean_grad - o_hat * mean_proj))
            dwout_ref[...] += nt_dot(o_norm, dup_ref[row])
            return carry

        lax.fori_loop(0, NR, chain, 0, unroll=4)
        lane = lax.broadcasted_iota(jnp.int32, (NB, 128), 1)
        low = lane < 64
        even = lane % 64 < 32

        def pack(ch, carry):
            base = pl.multiple_of(ch * SO, 8)
            val = o_scr[0, pl.ds(base, NR), :]
            do_ref[ch] = jnp.where(first_core, val, pltpu.roll(val, 64, 1)).astype(BF16)
            g0, g1, g2, g3 = (val[NB * g:NB * (g + 1)] for g in range(4))
            r0, r1, r2, r3 = (pltpu.roll(g, 64, 1) for g in (g0, g1, g2, g3))
            a0, a1 = jnp.where(low, g0, r2), jnp.where(low, g1, r3)
            a2, a3 = jnp.where(low, r0, g2), jnp.where(low, r1, g3)
            p0 = jnp.where(even, a0, pltpu.roll(a1, 32, 1))
            p1 = jnp.where(even, pltpu.roll(a0, 96, 1), a1)
            p2 = jnp.where(even, a2, pltpu.roll(a3, 32, 1))
            p3 = jnp.where(even, pltpu.roll(a2, 96, 1), a3)
            same0[ch] = jnp.where(first_core, p0, p2).astype(BF16)
            same1[ch] = jnp.where(first_core, p1, p3).astype(BF16)
            cross0[ch] = jnp.where(first_core, p2, p0).astype(BF16)
            cross1[ch] = jnp.where(first_core, p3, p1).astype(BF16)
            return carry

        lax.fori_loop(0, C, pack, 0, unroll=4)


def piece_spec(width, blk):
    return pl.BlockSpec((width, HALF, N), lambda s, *ids: (s, blk, 0))


def out_call(chunk, ids, a_own, b_pieces, don, dup, g1, w_out_t, scale, offset):
    lane_spec = pl.BlockSpec((NR, C, 128), lambda s, ids: (0, 0, chunk))
    acc_spec = full_spec((C, 128))
    pack_spec = full_spec((C, NB, 128))
    return pl.pallas_call(
        out_kernel,
        grid_spec=pltpu.PrefetchScalarGridSpec(
            num_scalar_prefetch=1,
            grid=(C // CB,),
            in_specs=[pl.BlockSpec((CB, NR, N), lambda s, ids: (s, 0, 0))] + [piece_spec(CB, blk) for _, blk in b_pieces]
            + [lane_spec, lane_spec, lane_spec, full_spec((C, C + 16)), full_spec((C, 128)), full_spec((C, 128))],
            out_specs=[full_spec((C, NR, 128)), full_spec((NR, C, 128))] + [pack_spec] * 4 + [acc_spec] * 3 + [TOKEN_SPEC],
            scratch_shapes=[pltpu.VMEM((1, C * SO, 128), F32)],
        ),
        out_shape=[sds((C, NR, 128), BF16), sds((NR, C, 128), BF16)] + [sds((C, NB, 128), BF16)] * 4 + [sds((C, 128), F32)] * 3 + [TOKEN],
        compiler_params=pltpu.CompilerParams(vmem_limit_bytes=VMEM_LIMIT),
        cost_estimate=pl.CostEstimate(flops=2 * 128 * 64 * 128 * 512, bytes_accessed=48 << 20, transcendentals=0),
        name="out_chain",
    )(ids, a_own, *(arr for arr, _ in b_pieces), don, dup, g1, w_out_t, scale, offset)


CK = 8


def da_kernel(*refs):
    do_refs, b_refs, da_ref = refs[:4], refs[4:20], refs[20]
    for ch in range(CK):
        do_row = jnp.concatenate([ref[ch] for ref in do_refs], axis=1)
        b_rows = jnp.concatenate([ref[ch] for ref in b_refs], axis=0)
        da_ref[ch] = nn_dot(do_row, b_rows).astype(BF16)


def da_call(do_chunks, b_pieces):
    return pl.pallas_call(
        da_kernel,
        grid=(C // CK,),
        in_specs=[pl.BlockSpec((CK, NR, 128), lambda s: (s, 0, 0))] * 4 + [piece_spec(CK, blk) for _, blk in b_pieces],
        out_specs=pl.BlockSpec((CK, NR, N), lambda s: (s, 0, 0)),
        out_shape=sds((C, NR, N), BF16),
        compiler_params=pltpu.CompilerParams(vmem_limit_bytes=VMEM_LIMIT),
        cost_estimate=pl.CostEstimate(flops=2 * 128 * 64 * 512 * 512, bytes_accessed=80 << 20, transcendentals=0),
        name="grad_a",
    )(*do_chunks, *(arr for arr, _ in b_pieces))


def db_kernel(*refs):
    do_refs, a_refs, db_ref = refs[:16], refs[16:32], refs[32]
    for ch in range(CK):
        x_t = [jnp.concatenate([ref[ch] for ref in do_refs[8 * h:8 * h + 8]], axis=0).T for h in range(2)]
        total = None
        for g in range(4):
            lhs = jnp.concatenate([x[32 * g:32 * g + 32] for x in x_t], axis=0)
            half, sub = divmod(g, 2)
            rhs = jnp.concatenate([ref[ch, NB * sub:NB * (sub + 1), :] for ref in a_refs[8 * half:8 * half + 8]], axis=0)
            term = nn_dot(lhs, rhs)
            total = term if total is None else total + term
        db_ref[ch] = total.astype(BF16)


def db_call(do_pieces, a_pieces):
    return pl.pallas_call(
        db_kernel,
        grid=(C // CK,),
        in_specs=[pl.BlockSpec((CK, NB, 128), lambda s: (s, 0, 0))] * 16 + [piece_spec(CK, blk) for _, blk in a_pieces],
        out_specs=pl.BlockSpec((CK, NR, N), lambda s: (s, 0, 0)),
        out_shape=sds((C, NR, N), BF16),
        compiler_params=pltpu.CompilerParams(vmem_limit_bytes=VMEM_LIMIT),
        cost_estimate=pl.CostEstimate(flops=2 * 128 * 64 * 512 * 512, bytes_accessed=80 << 20, transcendentals=0),
        name="grad_b",
    )(*do_pieces, *(arr for arr, _ in a_pieces))


def in_kernel(ids_ref, z_ref, dy_ref, m_ref, da_ref, db_ref, dg0, dg1, dg2, dg3, w_ref, scale_ref, offset_ref, w_cat_ref,
              dz_ref, dw_ref, dbin_ref, dsc_ref, doff_ref, a_scr, b_scr, m_scr):
    @pl.when(pl.program_id(0) == 0)
    def _():
        dw_ref[...] = jnp.zeros_like(dw_ref)
        dbin_ref[...] = jnp.zeros_like(dbin_ref)
        dsc_ref[...] = jnp.zeros_like(dsc_ref)
        doff_ref[...] = jnp.zeros_like(doff_ref)

    def unpack(ch, carry):
        base = pl.multiple_of(ch * SB, 8)
        for src, scr in ((da_ref, a_scr), (db_ref, b_scr)):
            for lane in range(4):
                scr[lane, pl.ds(base, NB), :] = src[ch, :, 128 * lane:128 * (lane + 1)].astype(F32)
        return carry

    lax.fori_loop(0, C, unpack, 0, unroll=4)

    load_mask(m_ref, m_scr, ids_ref)
    first = pl.program_id(0) % 2 * NB

    def body(row, carry):
        x_hat, inv_std, z_norm = normed_row(pair_row(z_ref, row, ids_ref), scale_ref[...], offset_ref[...])
        aug = jnp.concatenate([z_norm, ones_rows(N)], axis=0)
        mask_f = m_scr[pl.ds(first + row, 1), :]
        parts = []
        for side, scr in ((0, a_scr), (1, b_scr)):
            proj = nn_dot(w_ref[side * C:(side + 1) * C], aug)
            sig = sigmoid(nn_dot(w_ref[(2 + side) * C:(3 + side) * C], aug))
            d_proj = get_row(scr, row, SB) * mask_f * sig
            d_lin = d_proj * proj * (1.0 - sig)
            dbin_ref[side * C:(side + 1) * C] += lanes(d_proj)
            dbin_ref[(2 + side) * C:(3 + side) * C] += lanes(d_lin)
            parts.append((d_proj.astype(BF16), d_lin.astype(BF16)))
        cat = jnp.concatenate([parts[0][0], parts[1][0], parts[0][1], parts[1][1], jnp.concatenate([dg[row] for dg in (dg0, dg1, dg2, dg3)], axis=1)], axis=0)
        dw_ref[...] += nt_dot(cat, z_norm)
        d_znorm = nn_dot(w_cat_ref[...], cat).astype(BF16).astype(F32)
        dsc_ref[...] += lanes(d_znorm * x_hat)
        doff_ref[...] += lanes(d_znorm)
        grad_hat = d_znorm * scale_ref[...]
        mean_grad = jnp.mean(grad_hat, axis=0, keepdims=True)
        mean_proj = jnp.mean(grad_hat * x_hat, axis=0, keepdims=True)
        d_zt = inv_std * (grad_hat - mean_grad - x_hat * mean_proj)
        d_row = (pair_row(dy_ref, row, ids_ref).astype(F32) + d_zt.T).astype(BF16)
        for p in range(16):
            dz_ref[row, pl.ds(pl.multiple_of(ids_ref[p], HALF), HALF), :] = d_row[HALF * p:HALF * (p + 1)]
        return carry

    lax.fori_loop(0, NB, body, 0, unroll=2)


def in_call(ids, z_loc, dy_loc, m_loc, d_a, d_b, dg_chunks, w_t, scale, offset, w_cat):
    row_spec = pl.BlockSpec((NB, N, C), lambda r, ids: (r, 0, 0))
    act_spec = pl.BlockSpec((C, NB, N), lambda r, ids: (0, r, 0))
    return pl.pallas_call(
        in_kernel,
        grid_spec=pltpu.PrefetchScalarGridSpec(
            num_scalar_prefetch=1,
            grid=(NQ,),
            in_specs=[row_spec, row_spec, pl.BlockSpec((1, N, C), lambda r, ids: (r // 2, 0, 0)), act_spec, act_spec]
            + [pl.BlockSpec((NB, C, 128), lambda r, ids: (r, 0, 0))] * 4
            + [full_spec((4 * C, C + 16)), full_spec((C, N)), full_spec((C, N)), full_spec((C, 5 * C))],
            out_specs=[row_spec, full_spec((5 * C, C)), full_spec((4 * C, 128)), full_spec((C, 128)), full_spec((C, 128))],
            scratch_shapes=[pltpu.VMEM((4, C * SB, 128), F32)] * 2 + [pltpu.VMEM((C, N), F32)],
        ),
        out_shape=[sds((NR, N, C), BF16), sds((5 * C, C), F32), sds((4 * C, 128), F32), sds((C, 128), F32), sds((C, 128), F32)],
        compiler_params=pltpu.CompilerParams(vmem_limit_bytes=VMEM_LIMIT),
        cost_estimate=pl.CostEstimate(flops=2 * 64 * 512 * 640 * 128 * 3, bytes_accessed=64 << 20, transcendentals=1 << 23),
        name="in_backward",
    )(ids, z_loc, dy_loc, m_loc, d_a, d_b, *dg_chunks, w_t, scale, offset, w_cat)


def aug_weight(w_mat, bias):
    wide = jnp.zeros((w_mat.shape[1], 16), BF16).at[:, 0].set(bias)
    return jnp.concatenate([w_mat.T, wide], axis=1)


def column(vec, width):
    return jnp.broadcast_to(vec.astype(F32)[:, None], (C, width))


def local_grads(z_loc, mask_loc, dy_loc, ln_in_scale, ln_in_offset, w_in, b_in, ln_out_scale, ln_out_offset, w_out, b_out, w_gate, b_gate):
    me = lax.axis_index('dap')
    chip, core = me // 2, me % 2
    w_cat = jnp.concatenate([w_in, w_gate], axis=1)
    w_t = aug_weight(w_cat, jnp.concatenate([b_in, b_gate]))
    w_out_t = aug_weight(w_out, b_out)
    in_scale, in_offset = column(ln_in_scale, N), column(ln_in_offset, N)
    out_scale, out_offset = column(ln_out_scale, 128), column(ln_out_offset, 128)

    order = [((chip * 2) ^ HOPS[q][h]) * NR + core_of * NR + h * HALF for q in range(4) for core_of in range(2) for h in range(2)]
    ids = jnp.stack(order + [core]).astype(jnp.int32)
    mask_t = jnp.transpose(mask_loc.reshape(2, HALF, N), (0, 2, 1)).astype(BF16)
    mask_t = jnp.pad(mask_t, ((0, 0), (0, 0), (0, C - HALF)))

    def move(val, flips):
        return lax.ppermute(val, 'dap', [(d, d ^ flips) for d in range(8)])

    top, bottom = (jnp.concatenate([z_loc[HALF * h:HALF * (h + 1)], mask_t[h:h + 1]], axis=0) for h in range(2))
    gathered = {}
    gathered[1, 0], gathered[1, 1] = move(top, HOPS[1][0]), move(bottom, HOPS[1][1])
    gathered[2, 0], gathered[2, 1] = move(gathered[1, 0], HOPS[1][1]), move(gathered[1, 1], HOPS[1][0])
    gathered[3, 0], gathered[3, 1] = move(top, HOPS[3][0]), move(bottom, HOPS[3][1])

    a_own, b_own, dup, don, g1, acc_bout, acc_ooff, ids = own_call(ids, z_loc, dy_loc, mask_t, w_t, in_scale, in_offset, w_out)
    b_par, a_par = move(b_own, 1), move(a_own, 1)
    a_at = {(0, h, f): (val, h) for h in range(2) for f, val in ((0, a_own), (1, a_par))}
    b_at = {(0, h, f): (val, h) for h in range(2) for f, val in ((0, b_own), (1, b_par))}
    do_at, do_chunks, dg_chunks, sums = {}, [], [], []
    for q in range(4):
        for h in range(2):
            if q:
                act_a, act_b, ids = gated_call(ids, gathered[q, h], w_t[:4 * C], in_scale, in_offset)
                a_at[q, h, 0], b_at[q, h, 0] = (act_a, 0), (act_b, 0)
                b_at[q, h, 1] = move(act_b, 1), 0
                a_at[q, h, 1] = move(act_a, 1), 0
        b_pieces = [b_at[q, h, f] for f in range(2) for h in range(2)]
        do_own, dg, same0, same1, cross0, cross1, *acc, ids = out_call(q, ids, a_own, b_pieces, don, dup, g1, w_out_t, out_scale, out_offset)
        do_chunks.append(do_own)
        dg_chunks.append(dg)
        sums.append(acc)
        for flip, h, val in ((0, 0, same0), (0, 1, same1), (1, 0, cross0), (1, 1, cross1)):
            flips = HOPS[q][h] ^ flip
            do_at[h, flips] = move(val, flips) if flips else val
    d_a = da_call(do_chunks, [b_at[q, h, f] for q in range(4) for f in range(2) for h in range(2)])
    chunk_of = {(HOPS[q][h], h): q for q in range(4) for h in range(2)}
    d_b = db_call([do_at[h, s] for h in range(2) for s in range(8)],
                  [a_at[chunk_of[s & 6, h], h, s & 1] for h in range(2) for s in range(8)])
    d_z, acc_w, acc_bin, acc_isc, acc_ioff = in_call(ids, z_loc, dy_loc, mask_t, d_a, d_b, dg_chunks, w_t[:4 * C], in_scale, in_offset, w_cat)

    acc_wout, acc_osc, acc_bg = (sum(s[n] for s in sums) for n in range(3))
    vecs = [jnp.sum(v, axis=1) for v in (acc_isc, acc_ioff, acc_bin, acc_osc, acc_ooff, acc_bout, acc_bg)]
    vecs, acc_w, acc_wout = lax.psum((jnp.concatenate(vecs), acc_w, acc_wout), 'dap')
    vecs = vecs.astype(BF16)
    d_isc, d_ioff, d_bin, d_osc, d_ooff, d_bout, d_bg = jnp.split(vecs, [C, 2 * C, 6 * C, 7 * C, 8 * C, 9 * C])
    acc_w = acc_w.T.astype(BF16)
    return d_z, d_isc, d_ioff, acc_w[:, :4 * C], d_bin, d_osc, d_ooff, acc_wout.astype(BF16), d_bout, acc_w[:, 4 * C:], d_bg


def solution(mesh):
    pair_spec = P(('batch', 'dap'), None, None)
    mask_spec = P(('batch', 'dap'), None)
    vec_rep = P(None)
    mat_rep = P(None, None)
    vec_part = P('batch')
    mat_part = P('batch', None)
    in_specs = (pair_spec, mask_spec, pair_spec, vec_rep, vec_rep, mat_rep, vec_rep, vec_rep, vec_rep, mat_rep, vec_rep, mat_rep, vec_rep)
    out_specs = (pair_spec, vec_part, vec_part, mat_part, vec_part, vec_part, vec_part, mat_part, vec_part, mat_part, vec_part)
    return jax.shard_map(local_grads, mesh=mesh, in_specs=in_specs, out_specs=out_specs, check_vma=False)
```

```python
import functools
import jax
import jax.numpy as jnp
from jax import lax
from jax.experimental import pallas as pl
from jax.experimental.pallas import tpu as pltpu
from jax.sharding import PartitionSpec as P

LN_EPS = 1e-5
N = 512
C = 128
NR = 64
NB = 16
NQ = NR // NB
HALF = NR // 2
HOPS = ((0, 0), (2, 4), (6, 6), (4, 2))
SB = NB + 4
SO = NR + 4
WIDE = N // 2
F32 = jnp.float32
BF16 = jnp.bfloat16
PARAMS = pltpu.CompilerParams(vmem_limit_bytes=60 << 20)
COST = pl.CostEstimate(flops=1 << 33, bytes_accessed=1 << 26, transcendentals=0)


def sds(shape, dtype):
    return jax.ShapeDtypeStruct(shape, dtype)


def full_spec(shape):
    return pl.BlockSpec(shape, lambda *ids: (0,) * len(shape))


def sigmoid(x_val):
    return 1.0 / (1.0 + jnp.exp(-x_val))


def nt_dot(lhs, rhs):
    return lax.dot_general(lhs, rhs, (((1,), (1,)), ((), ())), preferred_element_type=F32)


def nn_dot(lhs, rhs):
    return lax.dot_general(lhs, rhs, (((1,), (0,)), ((), ())), preferred_element_type=F32)


def ones_rows(width):
    return jnp.where(lax.broadcasted_iota(jnp.int32, (16, width), 0) == 0, 1.0, 0.0).astype(BF16)


def norm_rows(x_val):
    mean_val = jnp.mean(x_val, axis=0, keepdims=True)
    centered = x_val - mean_val
    inv_std = lax.rsqrt(jnp.mean(centered * centered, axis=0, keepdims=True) + LN_EPS)
    return centered * inv_std, inv_std


def put_row(scr, row, pitch, val, lane=0):
    for tile in jnp.split(val, val.shape[1] // C, axis=1):
        scr[lane, pl.ds(row, C, stride=pitch), :] = tile
        lane += 1


def get_row(scr, row, pitch, lanes):
    return jnp.concatenate([scr[lane, pl.ds(row, C, stride=pitch), :] for lane in lanes], axis=1)


def flush_rows(scr, out_ref):
    def body(ch, carry):
        for lane in range(4):
            out_ref[ch, :, C * lane:C * (lane + 1)] = scr[lane, pl.ds(ch * SB, NB), :].astype(BF16)
        return carry

    lax.fori_loop(0, C, body, 0, unroll=8)


def gated_half(w_ref, scrs, row, half, z_norm, mask_f):
    aug = jnp.concatenate([z_norm, ones_rows(WIDE)], axis=0)
    for side, scr in enumerate(scrs):
        proj = nn_dot(w_ref[2 * C * side:2 * C * (side + 1)], aug)
        put_row(scr, row, SB, mask_f * sigmoid(proj[C:]) * proj[:C], 2 * half)
    return aug


def halves():
    return ((half, slice(WIDE * half, WIDE * (half + 1))) for half in range(2))


def pair_row(ref, row, ids_ref, half):
    return jnp.concatenate([ref[row, pl.ds(pl.multiple_of(ids_ref[8 * half + p], HALF), HALF), :] for p in range(8)], axis=0)


def normed_row(z_row, scale, offset):
    z_t = z_row.T.astype(F32)
    x_hat, inv_std = norm_rows(z_t)
    z_norm = (x_hat * scale + offset).astype(BF16)
    return x_hat, inv_std, z_norm


def pass_ids(ids_ref, tok_ref):
    for p in range(17):
        tok_ref[p] = ids_ref[p]


TOKEN = sds((17,), jnp.int32)
TOKEN_SPEC = pl.BlockSpec(memory_space=pltpu.SMEM)


def load_mask(m_ref, m_scr, ids_ref):
    for half, cols in halves():
        m_scr[:, cols] = pair_row(m_ref, 0, ids_ref, half).astype(F32).T


def gated_kernel(half_id, ids_ref, z_ref, m_ref, w_ref, scale_ref, offset_ref, a_ref, b_ref, tok_ref, a_scr, b_scr, m_scr):
    pass_ids(ids_ref, tok_ref)
    load_mask(m_ref, m_scr, ids_ref)
    first = half_id * HALF + pl.program_id(0) * NB

    def body(row, carry):
        for half, cols in halves():
            _, _, z_norm = normed_row(pair_row(z_ref, row, ids_ref, half), scale_ref[...], offset_ref[...])
            gated_half(w_ref, (a_scr, b_scr), row, half, z_norm, m_scr[pl.ds(first + row, 1), cols])
        return carry

    lax.fori_loop(0, NB, body, 0, unroll=4)
    flush_rows(a_scr, a_ref)
    flush_rows(b_scr, b_ref)


def gated_call(half_id, ids, piece, mask_t, w_t, scale, offset):
    out_spec = pl.BlockSpec((C, NB, N), lambda r, ids: (0, r, 0))
    return pl.pallas_call(
        functools.partial(gated_kernel, half_id),
        grid_spec=pltpu.PrefetchScalarGridSpec(
            num_scalar_prefetch=1,
            grid=(HALF // NB,),
            in_specs=[
                pl.BlockSpec((NB, N, C), lambda r, ids: (r, 0, 0)),
                full_spec((1, N, C)),
                full_spec((4 * C, C + 16)), full_spec((C, WIDE)), full_spec((C, WIDE)),
            ],
            out_specs=[out_spec, out_spec, TOKEN_SPEC],
            scratch_shapes=[pltpu.VMEM((4, C * SB, 128), F32)] * 2 + [pltpu.VMEM((C, N), F32)],
        ),
        out_shape=[sds((C, HALF, N), BF16)] * 2 + [TOKEN],
        compiler_params=PARAMS,
        cost_estimate=COST,
        name="gated_rows",
    )(ids, piece, mask_t, w_t, scale, offset)


def lanes(val):
    half = val.shape[1] // 2
    return val[:, :half] + val[:, half:]


def own_kernel(ids_ref, z_ref, dy_ref, m_ref, w_ref, scale_ref, offset_ref, w_out_ref,
               a_ref, b_ref, dup_ref, don_ref, g1_ref, dbout_ref, dooff_ref, tok_ref, a_scr, b_scr, m_scr):
    pass_ids(ids_ref, tok_ref)

    @pl.when(pl.program_id(0) == 0)
    def _():
        dbout_ref[...] = jnp.zeros_like(dbout_ref)
        dooff_ref[...] = jnp.zeros_like(dooff_ref)

    load_mask(m_ref, m_scr, ids_ref)
    first = pl.program_id(0) * NB

    def body(row, carry):
        for half, cols in halves():
            _, _, z_norm = normed_row(pair_row(z_ref, row, ids_ref, half), scale_ref[...], offset_ref[...])
            aug = gated_half(w_ref, (a_scr, b_scr), row, half, z_norm, m_scr[pl.ds(first + row, 1), cols])
            sig_g = sigmoid(nn_dot(w_ref[4 * C:5 * C], aug))
            d_upd = sig_g * pair_row(dy_ref, row, ids_ref, half).T.astype(F32)
            g1_ref[row, :, cols] = d_upd * (1.0 - sig_g)
            d_upd16 = d_upd.astype(BF16)
            dup_ref[row, :, cols] = d_upd16
            d_onorm = nn_dot(w_out_ref[...], d_upd16).astype(BF16)
            don_ref[row, :, cols] = d_onorm
            dbout_ref[...] += lanes(d_upd16.astype(F32))
            dooff_ref[...] += lanes(d_onorm.astype(F32))
        return carry

    lax.fori_loop(0, NB, body, 0, unroll=4)
    flush_rows(a_scr, a_ref)
    flush_rows(b_scr, b_ref)


def own_call(ids, z_loc, dy_loc, m_loc, w_t, scale, offset, w_out):
    row_spec = pl.BlockSpec((NB, N, C), lambda r, ids: (r, 0, 0))
    t_spec = pl.BlockSpec((NB, C, N), lambda r, ids: (r, 0, 0))
    act_spec = pl.BlockSpec((C, NB, N), lambda r, ids: (0, r, 0))
    return pl.pallas_call(
        own_kernel,
        grid_spec=pltpu.PrefetchScalarGridSpec(
            num_scalar_prefetch=1,
            grid=(NQ,),
            in_specs=[row_spec, row_spec, full_spec((1, N, C)),
                      full_spec((5 * C, C + 16)), full_spec((C, WIDE)), full_spec((C, WIDE)), full_spec((C, C))],
            out_specs=[act_spec, act_spec, t_spec, t_spec, t_spec, full_spec((C, 128)), full_spec((C, 128)), TOKEN_SPEC],
            scratch_shapes=[pltpu.VMEM((4, C * SB, 128), F32)] * 2 + [pltpu.VMEM((C, N), F32)],
        ),
        out_shape=[sds((C, NR, N), BF16), sds((C, NR, N), BF16), sds((NR, C, N), BF16), sds((NR, C, N), BF16), sds((NR, C, N), F32), sds((C, 128), F32), sds((C, 128), F32), TOKEN],
        compiler_params=PARAMS,
        cost_estimate=COST,
        name="own_rows",
    )(ids, z_loc, dy_loc, m_loc, w_t, scale, offset, w_out)


CB = 16
CP = 32
FIRST = C // CB
LAST = FIRST + NR // NB


def out_kernel(ids_ref, a_ref, b_own0, b_own1, b_par0, b_par1, don_ref, dup_ref, g1_ref, w_out_ref, scale_ref, offset_ref,
               do_ref, dg_ref, same0, same1, cross0, cross1, dwout_ref, dosc_ref, dbg_ref, tok_ref, o_scr):
    step = pl.program_id(0)
    first_core = ids_ref[16] == 0

    @pl.when(step == 0)
    def _():
        pass_ids(ids_ref, tok_ref)
        dwout_ref[...] = jnp.zeros_like(dwout_ref)
        dosc_ref[...] = jnp.zeros_like(dosc_ref)
        dbg_ref[...] = jnp.zeros_like(dbg_ref)

    @pl.when(step < FIRST)
    def _():
        def prod(ch, carry):
            b_rows = jnp.concatenate([ref[ch] for ref in (b_own0, b_own1, b_par0, b_par1)], axis=0)
            val = nt_dot(a_ref[ch], b_rows)
            o_scr[0, pl.ds((step * CB + ch) * SO, NR), :] = jnp.where(first_core, val, pltpu.roll(val, 64, 1))
            return carry

        lax.fori_loop(0, CB, prod, 0, unroll=8)

    @pl.when((step >= FIRST) & (step < LAST))
    def _():
        def chain(row, carry):
            o_row = (step - FIRST) * NB + row
            o_hat, inv_std = norm_rows(get_row(o_scr, o_row, SO, (0,)))
            o_norm = (o_hat * scale_ref[...] + offset_ref[...]).astype(BF16)
            aug = jnp.concatenate([o_norm, ones_rows(C)], axis=0)
            upd = nn_dot(w_out_ref[...], aug).astype(BF16).astype(F32)
            d_gate = g1_ref[row] * upd
            dbg_ref[...] += d_gate
            dg_ref[row] = d_gate.astype(BF16)
            d_onorm = don_ref[row].astype(F32)
            dosc_ref[...] += d_onorm * o_hat
            grad_hat = d_onorm * scale_ref[...]
            mean_grad = jnp.mean(grad_hat, axis=0, keepdims=True)
            mean_proj = jnp.mean(grad_hat * o_hat, axis=0, keepdims=True)
            put_row(o_scr, o_row, SO, inv_std * (grad_hat - mean_grad - o_hat * mean_proj))
            dwout_ref[...] += nt_dot(o_norm, dup_ref[row])
            return carry

        lax.fori_loop(0, NB, chain, 0, unroll=8)

    @pl.when(step >= LAST)
    def _():
        lane = lax.broadcasted_iota(jnp.int32, (NB, C), 1)
        low = lane < 64
        even = lane % 64 < HALF

        def swap(left, right, keep, width):
            return jnp.where(keep, left, pltpu.roll(right, width, 1)), jnp.where(keep, pltpu.roll(left, C - width, 1), right)

        def pack(ch, carry):
            val = o_scr[0, pl.ds(((step - LAST) * CP + ch) * SO, NR), :]
            do_ref[ch] = jnp.where(first_core, val, pltpu.roll(val, 64, 1)).astype(BF16)
            g0, g1, g2, g3 = jnp.split(val, 4, axis=0)
            g0, g2 = swap(g0, g2, low, 64)
            g1, g3 = swap(g1, g3, low, 64)
            g0, g1 = swap(g0, g1, even, HALF)
            g2, g3 = swap(g2, g3, even, HALF)
            same0[ch] = jnp.where(first_core, g0, g2).astype(BF16)
            same1[ch] = jnp.where(first_core, g1, g3).astype(BF16)
            cross0[ch] = jnp.where(first_core, g2, g0).astype(BF16)
            cross1[ch] = jnp.where(first_core, g3, g1).astype(BF16)
            return carry

        lax.fori_loop(0, CP, pack, 0, unroll=4)


def piece_spec(width, blk):
    return pl.BlockSpec((width, HALF, N), lambda s, *ids: (s, blk, 0))


def prod_step(step):
    return jnp.minimum(step, FIRST - 1)


def chain_step(step):
    return jnp.clip(step - FIRST, 0, NR // NB - 1)


def pack_step(step):
    return jnp.clip(step - LAST, 0, C // CP - 1)


def out_call(chunk, ids, a_own, b_pieces, don, dup, g1, w_out_t, scale, offset):
    lane_spec = pl.BlockSpec((NB, C, C), lambda s, ids: (chain_step(s), 0, chunk))
    acc_spec = full_spec((C, C))
    pack_spec = pl.BlockSpec((CP, NB, C), lambda s, ids: (pack_step(s), 0, 0))
    b_specs = [pl.BlockSpec((CB, HALF, N), lambda s, ids, blk=blk: (prod_step(s), blk, 0)) for _, blk in b_pieces]
    return pl.pallas_call(
        out_kernel,
        grid_spec=pltpu.PrefetchScalarGridSpec(
            num_scalar_prefetch=1,
            grid=(LAST + C // CP,),
            in_specs=[pl.BlockSpec((CB, NR, N), lambda s, ids: (prod_step(s), 0, 0))] + b_specs
            + [lane_spec, lane_spec, lane_spec, full_spec((C, C + 16)), acc_spec, acc_spec],
            out_specs=[pl.BlockSpec((CP, NR, C), lambda s, ids: (pack_step(s), 0, 0)),
                       pl.BlockSpec((NB, C, C), lambda s, ids: (chain_step(s), 0, 0))] + [pack_spec] * 4 + [acc_spec] * 3 + [TOKEN_SPEC],
            scratch_shapes=[pltpu.VMEM((1, C * SO, C), F32)],
        ),
        out_shape=[sds((C, NR, C), BF16), sds((NR, C, C), BF16)] + [sds((C, NB, C), BF16)] * 4 + [sds((C, C), F32)] * 3 + [TOKEN],
        compiler_params=PARAMS,
        cost_estimate=COST,
        name="out_chain",
    )(ids, a_own, *(arr for arr, _ in b_pieces), don, dup, g1, w_out_t, scale, offset)


CK = 16


def da_kernel(*refs):
    do_refs, b_refs, da_ref = refs[:4], refs[4:20], refs[20]
    for ch in range(CK):
        do_row = jnp.concatenate([ref[ch] for ref in do_refs], axis=1)
        b_rows = jnp.concatenate([ref[ch] for ref in b_refs], axis=0)
        da_ref[ch] = nn_dot(do_row, b_rows).astype(BF16)


def da_call(do_chunks, b_pieces):
    return pl.pallas_call(
        da_kernel,
        grid=(C // CK,),
        in_specs=[pl.BlockSpec((CK, NR, 128), lambda s: (s, 0, 0))] * 4 + [piece_spec(CK, blk) for _, blk in b_pieces],
        out_specs=pl.BlockSpec((CK, NR, N), lambda s: (s, 0, 0)),
        out_shape=sds((C, NR, N), BF16),
        compiler_params=PARAMS,
        cost_estimate=COST,
        name="grad_a",
    )(*do_chunks, *(arr for arr, _ in b_pieces))


def db_kernel(*refs):
    do_refs, a_refs, db_ref = refs[:16], refs[16:32], refs[32]
    for ch in range(CK):
        x_t = [jnp.concatenate([ref[ch] for ref in do_refs[8 * h:8 * h + 8]], axis=0).T for h in range(2)]
        total = None
        for g in range(4):
            lhs = jnp.concatenate([x[32 * g:32 * g + 32] for x in x_t], axis=0)
            half, sub = divmod(g, 2)
            rhs = jnp.concatenate([ref[ch, NB * sub:NB * (sub + 1), :] for ref in a_refs[8 * half:8 * half + 8]], axis=0)
            term = nn_dot(lhs, rhs)
            total = term if total is None else total + term
        db_ref[ch] = total.astype(BF16)


def db_call(do_pieces, a_pieces):
    return pl.pallas_call(
        db_kernel,
        grid=(C // CK,),
        in_specs=[pl.BlockSpec((CK, NB, 128), lambda s: (s, 0, 0))] * 16 + [piece_spec(CK, blk) for _, blk in a_pieces],
        out_specs=pl.BlockSpec((CK, NR, N), lambda s: (s, 0, 0)),
        out_shape=sds((C, NR, N), BF16),
        compiler_params=PARAMS,
        cost_estimate=COST,
        name="grad_b",
    )(*do_pieces, *(arr for arr, _ in a_pieces))


def in_kernel(ids_ref, z_ref, dy_ref, m_ref, da_ref, db_ref, dg0, dg1, dg2, dg3, w_ref, scale_ref, offset_ref, w_cat_ref,
              dz_ref, dw_ref, dbin_ref, dsc_ref, doff_ref, a_scr, b_scr, m_scr):
    dgs = (dg0, dg1, dg2, dg3)

    @pl.when(pl.program_id(0) == 0)
    def _():
        dw_ref[...] = jnp.zeros_like(dw_ref)
        dbin_ref[...] = jnp.zeros_like(dbin_ref)
        dsc_ref[...] = jnp.zeros_like(dsc_ref)
        doff_ref[...] = jnp.zeros_like(doff_ref)

    def unpack(ch, carry):
        for src, scr in ((da_ref, a_scr), (db_ref, b_scr)):
            for lane in range(4):
                scr[lane, pl.ds(ch * SB, NB), :] = src[ch, :, C * lane:C * (lane + 1)].astype(F32)
        return carry

    lax.fori_loop(0, C, unpack, 0, unroll=4)

    load_mask(m_ref, m_scr, ids_ref)
    first = pl.program_id(0) * NB

    def lanes4(val):
        return lanes(lanes(val))

    def body(row, carry):
        def full_row(ref):
            return jnp.concatenate([pair_row(ref, row, ids_ref, half) for half in range(2)], axis=0)

        x_hat, inv_std, z_norm = normed_row(full_row(z_ref), scale_ref[...], offset_ref[...])
        aug = jnp.concatenate([z_norm, ones_rows(N)], axis=0)
        mask_f = m_scr[pl.ds(first + row, 1), :]
        parts = []
        for side, scr in ((0, a_scr), (1, b_scr)):
            proj = nn_dot(w_ref[2 * C * side:2 * C * side + C], aug)
            sig = sigmoid(nn_dot(w_ref[2 * C * side + C:2 * C * (side + 1)], aug))
            d_proj = get_row(scr, row, SB, range(4)) * mask_f * sig
            d_lin = d_proj * proj * (1.0 - sig)
            dbin_ref[side] += lanes4(d_proj)
            dbin_ref[2 + side] += lanes4(d_lin)
            parts.append((d_proj.astype(BF16), d_lin.astype(BF16)))
        d_gate = jnp.concatenate([dg[row] for dg in dgs], axis=1)
        cat = jnp.concatenate([part[kind] for kind in range(2) for part in parts] + [d_gate], axis=0)
        dw_ref[...] += nt_dot(cat, z_norm)
        d_znorm = nn_dot(w_cat_ref[...], cat).astype(BF16).astype(F32)
        dsc_ref[...] += lanes4(d_znorm * x_hat)
        doff_ref[...] += lanes4(d_znorm)
        grad_hat = d_znorm * scale_ref[...]
        mean_grad = jnp.mean(grad_hat, axis=0, keepdims=True)
        mean_proj = jnp.mean(grad_hat * x_hat, axis=0, keepdims=True)
        d_zt = inv_std * (grad_hat - mean_grad - x_hat * mean_proj)
        d_row = (full_row(dy_ref).astype(F32) + d_zt.T).astype(BF16)
        for p in range(16):
            dz_ref[row, pl.ds(pl.multiple_of(ids_ref[p], HALF), HALF), :] = d_row[HALF * p:HALF * (p + 1)]
        return carry

    lax.fori_loop(0, NB, body, 0, unroll=4)


def in_call(ids, z_loc, dy_loc, m_loc, d_a, d_b, dg_chunks, w_t, scale, offset, w_cat):
    row_spec = pl.BlockSpec((NB, N, C), lambda r, ids: (r, 0, 0))
    act_spec = pl.BlockSpec((C, NB, N), lambda r, ids: (0, r, 0))
    return pl.pallas_call(
        in_kernel,
        grid_spec=pltpu.PrefetchScalarGridSpec(
            num_scalar_prefetch=1,
            grid=(NQ,),
            in_specs=[row_spec, row_spec, full_spec((1, N, C)), act_spec, act_spec]
            + [pl.BlockSpec((NB, C, 128), lambda r, ids: (r, 0, 0))] * 4
            + [full_spec((4 * C, C + 16)), full_spec((C, N)), full_spec((C, N)), full_spec((C, 5 * C))],
            out_specs=[row_spec, full_spec((5 * C, C)), full_spec((4, C, C)), full_spec((C, 128)), full_spec((C, 128))],
            scratch_shapes=[pltpu.VMEM((4, C * SB, 128), F32)] * 2 + [pltpu.VMEM((C, N), F32)],
        ),
        out_shape=[sds((NR, N, C), BF16), sds((5 * C, C), F32), sds((4, C, C), F32), sds((C, 128), F32), sds((C, 128), F32)],
        compiler_params=PARAMS,
        cost_estimate=COST,
        name="in_backward",
    )(ids, z_loc, dy_loc, m_loc, d_a, d_b, *dg_chunks, w_t, scale, offset, w_cat)


SHARD = 112
VECS = 6 * C


def sum_kernel(*refs):
    accs, wout_refs, w_ref = refs[:7], refs[7:11], refs[11]
    win_ref, wgate_ref, wout_ref, vec_ref, src, recv, mine, total, send1, recv1, send2, recv2 = refs[12:]
    me = lax.axis_index('dap')

    def peer(step):
        return {'dap': lax.rem(me + step, 8)}

    barrier = pltpu.get_barrier_semaphore()
    for step in range(1, 8):
        pl.semaphore_signal(barrier, inc=1, device_id=peer(step), device_id_type=pl.DeviceIdType.MESH)
    for blk in range(5):
        src[C * blk:C * (blk + 1)] = w_ref[C * blk:C * (blk + 1)].T
    src[5 * C:VECS] = sum(ref[...] for ref in wout_refs[1:]) + wout_refs[0][...]
    rows = []
    for ref in accs:
        rows += [ref[n] for n in range(4)] if len(ref.shape) > 2 else [ref[...]]
    rows = [jnp.sum(val.T, axis=0, keepdims=True) for val in rows]
    src[VECS:] = jnp.concatenate(rows + [jnp.zeros((8 * SHARD - VECS - len(rows), C), F32)], axis=0)
    pl.semaphore_wait(barrier, 7)

    def shard(owner):
        return pl.ds(pl.multiple_of(owner * SHARD, 16), SHARD)

    copies = []
    for step in range(1, 8):
        copy = pltpu.make_async_remote_copy(
            src_ref=src.at[shard(lax.rem(me + step, 8))], dst_ref=recv.at[step], send_sem=send1.at[step], recv_sem=recv1.at[step],
            device_id=peer(step), device_id_type=pl.DeviceIdType.MESH)
        copy.start()
        copies.append(copy)
    val = src[shard(me), :]
    for step, copy in enumerate(copies):
        copy.wait()
        val += recv[step + 1]
    mine[...] = val.astype(BF16)
    total[shard(me), :] = val.astype(BF16)
    copies = []
    for step in range(1, 8):
        copy = pltpu.make_async_remote_copy(
            src_ref=mine, dst_ref=total.at[shard(me)], send_sem=send2.at[step], recv_sem=recv2.at[step],
            device_id=peer(step), device_id_type=pl.DeviceIdType.MESH)
        copy.start()
        copies.append(copy)
    for copy in copies:
        copy.wait()
    for blk in range(4):
        win_ref[:, C * blk:C * (blk + 1)] = total[C * blk:C * (blk + 1)]
    wgate_ref[...] = total[4 * C:5 * C]
    wout_ref[...] = total[5 * C:VECS]
    vec_ref[...] = total[VECS:VECS + 16]


def sum_call(accs, wouts, acc_w):
    args = [*accs, *wouts, acc_w]
    outs = [sds((C, 4 * C), BF16), sds((C, C), BF16), sds((C, C), BF16), sds((16, C), BF16)]
    return pl.pallas_call(
        sum_kernel,
        in_specs=[pl.BlockSpec(memory_space=pltpu.VMEM)] * len(args),
        out_specs=[pl.BlockSpec(memory_space=pltpu.VMEM)] * len(outs),
        out_shape=outs,
        scratch_shapes=[pltpu.VMEM((8 * SHARD, C), F32), pltpu.VMEM((8, SHARD, C), F32), pltpu.VMEM((SHARD, C), BF16), pltpu.VMEM((8 * SHARD, C), BF16)]
        + [pltpu.SemaphoreType.DMA((8,))] * 4,
        compiler_params=pltpu.CompilerParams(collective_id=0, has_side_effects=True),
        cost_estimate=COST,
        name="sum_grads",
    )(*args)


def aug_weight(w_mat, bias):
    wide = jnp.zeros((w_mat.shape[1], 16), BF16).at[:, 0].set(bias)
    return jnp.concatenate([w_mat.T, wide], axis=1)


def column(vec, width):
    return jnp.broadcast_to(vec.astype(F32)[:, None], (C, width))


def local_grads(z_loc, mask_loc, dy_loc, ln_in_scale, ln_in_offset, w_in, b_in, ln_out_scale, ln_out_offset, w_out, b_out, w_gate, b_gate):
    me = lax.axis_index('dap')
    chip, core = me // 2, me % 2
    w_cat = jnp.concatenate([w_in, w_gate], axis=1)
    pa, pb, la, lb, gate = jnp.split(jnp.concatenate([w_cat, jnp.concatenate([b_in, b_gate])[None]], axis=0), 5, axis=1)
    w_t = jnp.concatenate([pa, la, pb, lb, gate], axis=1)
    w_t = aug_weight(w_t[:C], w_t[C])
    w_out_t = aug_weight(w_out, b_out)
    (in_scale, in_offset), wide_in = ((column(ln_in_scale, width), column(ln_in_offset, width)) for width in (WIDE, N))
    out_scale, out_offset = column(ln_out_scale, 128), column(ln_out_offset, 128)

    order = [((chip * 2) ^ HOPS[q][h]) * NR + core_of * NR + h * HALF for q in range(4) for core_of in range(2) for h in range(2)]
    ids = jnp.stack(order + [core]).astype(jnp.int32)
    mask_t = jnp.pad(mask_loc.T.astype(BF16), ((0, 0), (0, C - NR)))[None]

    def move(val, flips):
        return lax.ppermute(val, 'dap', [(d, d ^ flips) for d in range(8)])

    top, bottom = z_loc[:HALF], z_loc[HALF:]
    gathered = {}
    gathered[1, 0], gathered[1, 1] = move(top, HOPS[1][0]), move(bottom, HOPS[1][1])
    masks = {hop: move(mask_t, hop) for hop in (2, 4, 6)}
    gathered[2, 0], gathered[2, 1] = move(gathered[1, 0], HOPS[1][1]), move(gathered[1, 1], HOPS[1][0])
    gathered[3, 0], gathered[3, 1] = move(top, HOPS[3][0]), move(bottom, HOPS[3][1])

    a_own, b_own, dup, don, g1, acc_bout, acc_ooff, ids = own_call(ids, z_loc, dy_loc, mask_t, w_t, in_scale, in_offset, w_out)
    b_par, a_par = move(b_own, 1), move(a_own, 1)
    a_at = {(0, h, f): (val, h) for h in range(2) for f, val in ((0, a_own), (1, a_par))}
    b_at = {(0, h, f): (val, h) for h in range(2) for f, val in ((0, b_own), (1, b_par))}
    do_at, do_chunks, dg_chunks, sums = {}, [], [], []
    for q in range(4):
        for h in range(2):
            if q:
                act_a, act_b, ids = gated_call(h, ids, gathered[q, h], masks[HOPS[q][h]], w_t[:4 * C], in_scale, in_offset)
                a_at[q, h, 0], b_at[q, h, 0] = (act_a, 0), (act_b, 0)
                b_at[q, h, 1] = move(act_b, 1), 0
                a_at[q, h, 1] = move(act_a, 1), 0
        b_pieces = [b_at[q, h, f] for f in range(2) for h in range(2)]
        do_own, dg, same0, same1, cross0, cross1, *acc, ids = out_call(q, ids, a_own, b_pieces, don, dup, g1, w_out_t, out_scale, out_offset)
        do_chunks.append(do_own)
        dg_chunks.append(dg)
        sums.append(acc)
        for flip, h, val in ((0, 0, same0), (0, 1, same1), (1, 0, cross0), (1, 1, cross1)):
            flips = HOPS[q][h] ^ flip
            do_at[h, flips] = move(val, flips) if flips else val
    d_a = da_call(do_chunks, [b_at[q, h, f] for q in range(4) for f in range(2) for h in range(2)])
    chunk_of = {(HOPS[q][h], h): q for q in range(4) for h in range(2)}
    d_b = db_call([do_at[h, s] for h in range(2) for s in range(8)],
                  [a_at[chunk_of[s & 6, h], h, s & 1] for h in range(2) for s in range(8)])
    d_z, acc_w, acc_bin, acc_isc, acc_ioff = in_call(ids, z_loc, dy_loc, mask_t, d_a, d_b, dg_chunks, w_t[:4 * C], *wide_in, w_cat)

    wouts, oscs, bgs = zip(*sums)
    accs = (acc_isc, acc_ioff, acc_bin, sum(oscs), acc_ooff, acc_bout, sum(bgs))
    d_win, d_wgate, d_wout, vecs = sum_call(accs, wouts, acc_w)
    d_isc, d_ioff, d_osc, d_ooff, d_bout, d_bg = (vecs[n] for n in (0, 1, 6, 7, 8, 9))
    return d_z, d_isc, d_ioff, d_win, vecs[2:6].reshape(4 * C), d_osc, d_ooff, d_wout, d_bout, d_wgate, d_bg


def solution(mesh):
    pair_spec = P(('batch', 'dap'), None, None)
    mask_spec = P(('batch', 'dap'), None)
    vec_rep = P(None)
    mat_rep = P(None, None)
    vec_part = P('batch')
    mat_part = P('batch', None)
    in_specs = (pair_spec, mask_spec, pair_spec, vec_rep, vec_rep, mat_rep, vec_rep, vec_rep, vec_rep, mat_rep, vec_rep, mat_rep, vec_rep)
    out_specs = (pair_spec, vec_part, vec_part, mat_part, vec_part, vec_part, vec_part, mat_part, vec_part, mat_part, vec_part)
    return jax.shard_map(local_grads, mesh=mesh, in_specs=in_specs, out_specs=out_specs, check_vma=False)
```

```python
import functools
import jax
import jax.numpy as jnp
from jax import lax
from jax.experimental import pallas as pl
from jax.experimental.pallas import tpu as pltpu
from jax.sharding import PartitionSpec as P

LN_EPS = 1e-5
N = 512
C = 128
NR = 64
NB = 16
NQ = NR // NB
HALF = NR // 2
HOPS = ((0, 0), (2, 4), (6, 6), (4, 2))
SB = NB + 4
SO = NR + 4
WIDE = N // 2
F32 = jnp.float32
BF16 = jnp.bfloat16
PARAMS = pltpu.CompilerParams(vmem_limit_bytes=60 << 20)
COST = pl.CostEstimate(flops=1 << 33, bytes_accessed=1 << 26, transcendentals=0)


def sds(shape, dtype):
    return jax.ShapeDtypeStruct(shape, dtype)


def full_spec(shape):
    return pl.BlockSpec(shape, lambda *ids: (0,) * len(shape))


def sigmoid(x_val):
    return 1.0 / (1.0 + jnp.exp(-x_val))


def nt_dot(lhs, rhs):
    return lax.dot_general(lhs, rhs, (((1,), (1,)), ((), ())), preferred_element_type=F32)


def nn_dot(lhs, rhs):
    return lax.dot_general(lhs, rhs, (((1,), (0,)), ((), ())), preferred_element_type=F32)


def ones_rows(width):
    return jnp.where(lax.broadcasted_iota(jnp.int32, (16, width), 0) == 0, 1.0, 0.0).astype(BF16)


def norm_rows(x_val):
    mean_val = jnp.mean(x_val, axis=0, keepdims=True)
    centered = x_val - mean_val
    inv_std = lax.rsqrt(jnp.mean(centered * centered, axis=0, keepdims=True) + LN_EPS)
    return centered * inv_std, inv_std


def put_row(scr, row, pitch, val, lane=0):
    for tile in jnp.split(val, val.shape[1] // C, axis=1):
        scr[lane, pl.ds(row, C, stride=pitch), :] = tile
        lane += 1


def get_row(scr, row, pitch, lanes):
    return jnp.concatenate([scr[lane, pl.ds(row, C, stride=pitch), :] for lane in lanes], axis=1)


def flush_rows(scr, out_ref):
    def body(ch, carry):
        for lane in range(4):
            out_ref[ch, :, C * lane:C * (lane + 1)] = scr[lane, pl.ds(ch * SB, NB), :].astype(BF16)
        return carry

    lax.fori_loop(0, C, body, 0, unroll=8)


def gated_half(w_ref, scrs, row, half, z_norm, mask_f):
    aug = jnp.concatenate([z_norm, ones_rows(WIDE)], axis=0)
    for side, scr in enumerate(scrs):
        proj = nn_dot(w_ref[2 * C * side:2 * C * (side + 1)], aug)
        put_row(scr, row, SB, mask_f * sigmoid(proj[C:]) * proj[:C], 2 * half)
    return aug


def halves():
    return ((half, slice(WIDE * half, WIDE * (half + 1))) for half in range(2))


def pair_row(ref, row, ids_ref, half):
    return jnp.concatenate([ref[row, pl.ds(pl.multiple_of(ids_ref[8 * half + p], HALF), HALF), :] for p in range(8)], axis=0)


def normed_row(z_row, scale, offset):
    z_t = z_row.T.astype(F32)
    x_hat, inv_std = norm_rows(z_t)
    z_norm = (x_hat * scale + offset).astype(BF16)
    return x_hat, inv_std, z_norm


def pass_ids(ids_ref, tok_ref):
    for p in range(17):
        tok_ref[p] = ids_ref[p]


TOKEN = sds((17,), jnp.int32)
TOKEN_SPEC = pl.BlockSpec(memory_space=pltpu.SMEM)


def load_mask(m_ref, m_scr, ids_ref):
    for half, cols in halves():
        m_scr[:, cols] = pair_row(m_ref, 0, ids_ref, half).astype(F32).T


def gated_kernel(half_id, ids_ref, z_ref, m_ref, w_ref, scale_ref, offset_ref, a_ref, b_ref, tok_ref, a_scr, b_scr, m_scr):
    pass_ids(ids_ref, tok_ref)
    load_mask(m_ref, m_scr, ids_ref)
    first = half_id * HALF + pl.program_id(0) * NB

    def body(row, carry):
        for half, cols in halves():
            _, _, z_norm = normed_row(pair_row(z_ref, row, ids_ref, half), scale_ref[...], offset_ref[...])
            gated_half(w_ref, (a_scr, b_scr), row, half, z_norm, m_scr[pl.ds(first + row, 1), cols])
        return carry

    lax.fori_loop(0, NB, body, 0, unroll=4)
    flush_rows(a_scr, a_ref)
    flush_rows(b_scr, b_ref)


def gated_call(half_id, ids, piece, mask_t, w_t, scale, offset):
    out_spec = pl.BlockSpec((C, NB, N), lambda r, ids: (0, r, 0))
    return pl.pallas_call(
        functools.partial(gated_kernel, half_id),
        grid_spec=pltpu.PrefetchScalarGridSpec(
            num_scalar_prefetch=1,
            grid=(HALF // NB,),
            in_specs=[
                pl.BlockSpec((NB, N, C), lambda r, ids: (r, 0, 0)),
                full_spec((1, N, C)),
                full_spec((4 * C, C + 16)), full_spec((C, WIDE)), full_spec((C, WIDE)),
            ],
            out_specs=[out_spec, out_spec, TOKEN_SPEC],
            scratch_shapes=[pltpu.VMEM((4, C * SB, 128), F32)] * 2 + [pltpu.VMEM((C, N), F32)],
        ),
        out_shape=[sds((C, HALF, N), BF16)] * 2 + [TOKEN],
        compiler_params=PARAMS,
        cost_estimate=COST,
        name="gated_rows",
    )(ids, piece, mask_t, w_t, scale, offset)


def lanes(val):
    half = val.shape[1] // 2
    return val[:, :half] + val[:, half:]


def own_kernel(ids_ref, z_ref, dy_ref, m_ref, w_ref, scale_ref, offset_ref, w_out_ref,
               a_ref, b_ref, dup_ref, don_ref, g1_ref, dbout_ref, dooff_ref, tok_ref, a_scr, b_scr, m_scr):
    pass_ids(ids_ref, tok_ref)

    @pl.when(pl.program_id(0) == 0)
    def _():
        dbout_ref[...] = jnp.zeros_like(dbout_ref)
        dooff_ref[...] = jnp.zeros_like(dooff_ref)

    load_mask(m_ref, m_scr, ids_ref)
    first = pl.program_id(0) * NB

    def body(row, carry):
        for half, cols in halves():
            _, _, z_norm = normed_row(pair_row(z_ref, row, ids_ref, half), scale_ref[...], offset_ref[...])
            aug = gated_half(w_ref, (a_scr, b_scr), row, half, z_norm, m_scr[pl.ds(first + row, 1), cols])
            sig_g = sigmoid(nn_dot(w_ref[4 * C:5 * C], aug))
            d_upd = sig_g * pair_row(dy_ref, row, ids_ref, half).T.astype(F32)
            g1_ref[row, :, cols] = d_upd * (1.0 - sig_g)
            d_upd16 = d_upd.astype(BF16)
            dup_ref[row, :, cols] = d_upd16
            d_onorm = nn_dot(w_out_ref[...], d_upd16).astype(BF16)
            don_ref[row, :, cols] = d_onorm
            dbout_ref[...] += lanes(d_upd16.astype(F32))
            dooff_ref[...] += lanes(d_onorm.astype(F32))
        return carry

    lax.fori_loop(0, NB, body, 0, unroll=4)
    flush_rows(a_scr, a_ref)
    flush_rows(b_scr, b_ref)


def own_call(ids, z_loc, dy_loc, m_loc, w_t, scale, offset, w_out):
    row_spec = pl.BlockSpec((NB, N, C), lambda r, ids: (r, 0, 0))
    t_spec = pl.BlockSpec((NB, C, N), lambda r, ids: (r, 0, 0))
    act_spec = pl.BlockSpec((C, NB, N), lambda r, ids: (0, r, 0))
    return pl.pallas_call(
        own_kernel,
        grid_spec=pltpu.PrefetchScalarGridSpec(
            num_scalar_prefetch=1,
            grid=(NQ,),
            in_specs=[row_spec, row_spec, full_spec((1, N, C)),
                      full_spec((5 * C, C + 16)), full_spec((C, WIDE)), full_spec((C, WIDE)), full_spec((C, C))],
            out_specs=[act_spec, act_spec, t_spec, t_spec, t_spec, full_spec((C, 128)), full_spec((C, 128)), TOKEN_SPEC],
            scratch_shapes=[pltpu.VMEM((4, C * SB, 128), F32)] * 2 + [pltpu.VMEM((C, N), F32)],
        ),
        out_shape=[sds((C, NR, N), BF16), sds((C, NR, N), BF16), sds((NR, C, N), BF16), sds((NR, C, N), BF16), sds((NR, C, N), F32), sds((C, 128), F32), sds((C, 128), F32), TOKEN],
        compiler_params=PARAMS,
        cost_estimate=COST,
        name="own_rows",
    )(ids, z_loc, dy_loc, m_loc, w_t, scale, offset, w_out)


CB = 32
CR = 32
CP = 64
FIRST = C // CB
LAST = FIRST + NR // CR


def out_kernel(ids_ref, a_ref, b_own0, b_own1, b_par0, b_par1, don_ref, dup_ref, g1_ref, w_out_ref, scale_ref, offset_ref,
               do_ref, dg_ref, same0, same1, cross0, cross1, dwout_ref, dosc_ref, dbg_ref, tok_ref, o_scr):
    step = pl.program_id(0)
    first_core = ids_ref[16] == 0

    @pl.when(step == 0)
    def _():
        pass_ids(ids_ref, tok_ref)
        dwout_ref[...] = jnp.zeros_like(dwout_ref)
        dosc_ref[...] = jnp.zeros_like(dosc_ref)
        dbg_ref[...] = jnp.zeros_like(dbg_ref)

    @pl.when(step < FIRST)
    def _():
        def prod(ch, carry):
            b_rows = jnp.concatenate([ref[ch] for ref in (b_own0, b_own1, b_par0, b_par1)], axis=0)
            val = nt_dot(a_ref[ch], b_rows)
            o_scr[0, pl.ds((step * CB + ch) * SO, NR), :] = jnp.where(first_core, val, pltpu.roll(val, 64, 1))
            return carry

        lax.fori_loop(0, CB, prod, 0, unroll=16)

    @pl.when((step >= FIRST) & (step < LAST))
    def _():
        def chain(row, carry):
            o_row = (step - FIRST) * CR + row
            o_hat, inv_std = norm_rows(get_row(o_scr, o_row, SO, (0,)))
            o_norm = (o_hat * scale_ref[...] + offset_ref[...]).astype(BF16)
            aug = jnp.concatenate([o_norm, ones_rows(C)], axis=0)
            upd = nn_dot(w_out_ref[...], aug).astype(BF16).astype(F32)
            d_gate = g1_ref[row] * upd
            dbg_ref[...] += d_gate
            dg_ref[row] = d_gate.astype(BF16)
            d_onorm = don_ref[row].astype(F32)
            dosc_ref[...] += d_onorm * o_hat
            grad_hat = d_onorm * scale_ref[...]
            mean_grad = jnp.mean(grad_hat, axis=0, keepdims=True)
            mean_proj = jnp.mean(grad_hat * o_hat, axis=0, keepdims=True)
            put_row(o_scr, o_row, SO, inv_std * (grad_hat - mean_grad - o_hat * mean_proj))
            dwout_ref[...] += nt_dot(o_norm, dup_ref[row])
            return carry

        lax.fori_loop(0, CR, chain, 0, unroll=8)

    @pl.when(step >= LAST)
    def _():
        lane = lax.broadcasted_iota(jnp.int32, (NB, C), 1)
        low = lane < 64
        even = lane % 64 < HALF

        def swap(left, right, keep, width):
            return jnp.where(keep, left, pltpu.roll(right, width, 1)), jnp.where(keep, pltpu.roll(left, C - width, 1), right)

        def pack(ch, carry):
            val = o_scr[0, pl.ds(((step - LAST) * CP + ch) * SO, NR), :]
            do_ref[ch] = jnp.where(first_core, val, pltpu.roll(val, 64, 1)).astype(BF16)
            g0, g1, g2, g3 = jnp.split(val, 4, axis=0)
            g0, g2 = swap(g0, g2, low, 64)
            g1, g3 = swap(g1, g3, low, 64)
            g0, g1 = swap(g0, g1, even, HALF)
            g2, g3 = swap(g2, g3, even, HALF)
            same0[ch] = jnp.where(first_core, g0, g2).astype(BF16)
            same1[ch] = jnp.where(first_core, g1, g3).astype(BF16)
            cross0[ch] = jnp.where(first_core, g2, g0).astype(BF16)
            cross1[ch] = jnp.where(first_core, g3, g1).astype(BF16)
            return carry

        lax.fori_loop(0, CP, pack, 0, unroll=8)


def piece_spec(width, blk):
    return pl.BlockSpec((width, HALF, N), lambda s, *ids: (s, blk, 0))


def prod_step(step):
    return jnp.minimum(step, FIRST - 1)


def chain_step(step):
    return jnp.clip(step - FIRST, 0, NR // CR - 1)


def pack_step(step):
    return jnp.clip(step - LAST, 0, C // CP - 1)


def out_call(chunk, ids, a_own, b_pieces, don, dup, g1, w_out_t, scale, offset):
    lane_spec = pl.BlockSpec((CR, C, C), lambda s, ids: (chain_step(s), 0, chunk))
    acc_spec = full_spec((C, C))
    pack_spec = pl.BlockSpec((CP, NB, C), lambda s, ids: (pack_step(s), 0, 0))
    b_specs = [pl.BlockSpec((CB, HALF, N), lambda s, ids, blk=blk: (prod_step(s), blk, 0)) for _, blk in b_pieces]
    return pl.pallas_call(
        out_kernel,
        grid_spec=pltpu.PrefetchScalarGridSpec(
            num_scalar_prefetch=1,
            grid=(LAST + C // CP,),
            in_specs=[pl.BlockSpec((CB, NR, N), lambda s, ids: (prod_step(s), 0, 0))] + b_specs
            + [lane_spec, lane_spec, lane_spec, full_spec((C, C + 16)), acc_spec, acc_spec],
            out_specs=[pl.BlockSpec((CP, NR, C), lambda s, ids: (pack_step(s), 0, 0)),
                       pl.BlockSpec((CR, C, C), lambda s, ids: (chain_step(s), 0, 0))] + [pack_spec] * 4 + [acc_spec] * 3 + [TOKEN_SPEC],
            scratch_shapes=[pltpu.VMEM((1, C * SO, C), F32)],
        ),
        out_shape=[sds((C, NR, C), BF16), sds((NR, C, C), BF16)] + [sds((C, NB, C), BF16)] * 4 + [sds((C, C), F32)] * 3 + [TOKEN],
        compiler_params=PARAMS,
        cost_estimate=COST,
        name="out_chain",
    )(ids, a_own, *(arr for arr, _ in b_pieces), don, dup, g1, w_out_t, scale, offset)


CK = 16


def da_kernel(count, *refs):
    do_refs, b_refs, da_ref = refs[:count], refs[count:5 * count], refs[-1]
    for ch in range(CK):
        do_row = jnp.concatenate([ref[ch] for ref in do_refs], axis=1)
        b_rows = jnp.concatenate([ref[ch] for ref in b_refs], axis=0)
        val = nn_dot(do_row, b_rows)
        for ref in refs[5 * count:-1]:
            val += ref[ch]
        da_ref[ch] = val.astype(da_ref.dtype)


def da_call(do_chunks, b_pieces, partial, dtype):
    row_spec = pl.BlockSpec((CK, NR, N), lambda s: (s, 0, 0))
    return pl.pallas_call(
        functools.partial(da_kernel, len(do_chunks)),
        grid=(C // CK,),
        in_specs=[pl.BlockSpec((CK, NR, C), lambda s: (s, 0, 0))] * len(do_chunks) + [piece_spec(CK, blk) for _, blk in b_pieces] + [row_spec] * len(partial),
        out_specs=row_spec,
        out_shape=sds((C, NR, N), dtype),
        compiler_params=PARAMS,
        cost_estimate=COST,
        name="grad_a",
    )(*do_chunks, *(arr for arr, _ in b_pieces), *partial)


def db_kernel(*refs):
    do_refs, a_refs, db_ref = refs[:16], refs[16:32], refs[32]
    for ch in range(CK):
        x_t = [jnp.concatenate([ref[ch] for ref in do_refs[8 * h:8 * h + 8]], axis=0).T for h in range(2)]
        total = None
        for g in range(4):
            lhs = jnp.concatenate([x[32 * g:32 * g + 32] for x in x_t], axis=0)
            half, sub = divmod(g, 2)
            rhs = jnp.concatenate([ref[ch, NB * sub:NB * (sub + 1), :] for ref in a_refs[8 * half:8 * half + 8]], axis=0)
            term = nn_dot(lhs, rhs)
            total = term if total is None else total + term
        db_ref[ch] = total.astype(BF16)


def db_call(do_pieces, a_pieces):
    return pl.pallas_call(
        db_kernel,
        grid=(C // CK,),
        in_specs=[pl.BlockSpec((CK, NB, 128), lambda s: (s, 0, 0))] * 16 + [piece_spec(CK, blk) for _, blk in a_pieces],
        out_specs=pl.BlockSpec((CK, NR, N), lambda s: (s, 0, 0)),
        out_shape=sds((C, NR, N), BF16),
        compiler_params=PARAMS,
        cost_estimate=COST,
        name="grad_b",
    )(*do_pieces, *(arr for arr, _ in a_pieces))


def in_kernel(ids_ref, z_ref, dy_ref, m_ref, da_ref, db_ref, dg0, dg1, dg2, dg3, w_ref, scale_ref, offset_ref, w_cat_ref,
              dz_ref, dw_ref, dbin_ref, dsc_ref, doff_ref, a_scr, b_scr, m_scr):
    dgs = (dg0, dg1, dg2, dg3)

    @pl.when(pl.program_id(0) == 0)
    def _():
        dw_ref[...] = jnp.zeros_like(dw_ref)
        dbin_ref[...] = jnp.zeros_like(dbin_ref)
        dsc_ref[...] = jnp.zeros_like(dsc_ref)
        doff_ref[...] = jnp.zeros_like(doff_ref)

    def unpack(ch, carry):
        for src, scr in ((da_ref, a_scr), (db_ref, b_scr)):
            for lane in range(4):
                scr[lane, pl.ds(ch * SB, NB), :] = src[ch, :, C * lane:C * (lane + 1)].astype(F32)
        return carry

    lax.fori_loop(0, C, unpack, 0, unroll=4)

    load_mask(m_ref, m_scr, ids_ref)
    first = pl.program_id(0) * NB

    def lanes4(val):
        return lanes(lanes(val))

    def body(row, carry):
        def full_row(ref):
            return jnp.concatenate([pair_row(ref, row, ids_ref, half) for half in range(2)], axis=0)

        x_hat, inv_std, z_norm = normed_row(full_row(z_ref), scale_ref[...], offset_ref[...])
        aug = jnp.concatenate([z_norm, ones_rows(N)], axis=0)
        mask_f = m_scr[pl.ds(first + row, 1), :]
        parts = []
        for side, scr in ((0, a_scr), (1, b_scr)):
            proj = nn_dot(w_ref[2 * C * side:2 * C * (side + 1)], aug)
            sig = sigmoid(proj[C:])
            d_proj = get_row(scr, row, SB, range(4)) * mask_f * sig
            d_lin = d_proj * proj[:C] * (1.0 - sig)
            dbin_ref[side] += lanes4(d_proj)
            dbin_ref[2 + side] += lanes4(d_lin)
            parts.append((d_proj.astype(BF16), d_lin.astype(BF16)))
        d_gate = jnp.concatenate([dg[row] for dg in dgs], axis=1)
        cat = jnp.concatenate([part[kind] for kind in range(2) for part in parts] + [d_gate], axis=0)
        dw_ref[...] += nt_dot(cat, z_norm)
        d_znorm = nn_dot(w_cat_ref[...], cat).astype(BF16).astype(F32)
        dsc_ref[...] += lanes4(d_znorm * x_hat)
        doff_ref[...] += lanes4(d_znorm)
        grad_hat = d_znorm * scale_ref[...]
        mean_grad = jnp.mean(grad_hat, axis=0, keepdims=True)
        mean_proj = jnp.mean(grad_hat * x_hat, axis=0, keepdims=True)
        d_zt = inv_std * (grad_hat - mean_grad - x_hat * mean_proj)
        d_row = (full_row(dy_ref).astype(F32) + d_zt.T).astype(BF16)
        for p in range(16):
            dz_ref[row, pl.ds(pl.multiple_of(ids_ref[p], HALF), HALF), :] = d_row[HALF * p:HALF * (p + 1)]
        return carry

    lax.fori_loop(0, NB, body, 0, unroll=4)


def in_call(ids, z_loc, dy_loc, m_loc, d_a, d_b, dg_chunks, w_t, scale, offset, w_cat):
    row_spec = pl.BlockSpec((NB, N, C), lambda r, ids: (r, 0, 0))
    act_spec = pl.BlockSpec((C, NB, N), lambda r, ids: (0, r, 0))
    return pl.pallas_call(
        in_kernel,
        grid_spec=pltpu.PrefetchScalarGridSpec(
            num_scalar_prefetch=1,
            grid=(NQ,),
            in_specs=[row_spec, row_spec, full_spec((1, N, C)), act_spec, act_spec]
            + [pl.BlockSpec((NB, C, 128), lambda r, ids: (r, 0, 0))] * 4
            + [full_spec((4 * C, C + 16)), full_spec((C, N)), full_spec((C, N)), full_spec((C, 5 * C))],
            out_specs=[row_spec, full_spec((5 * C, C)), full_spec((4, C, C)), full_spec((C, 128)), full_spec((C, 128))],
            scratch_shapes=[pltpu.VMEM((4, C * SB, 128), F32)] * 2 + [pltpu.VMEM((C, N), F32)],
        ),
        out_shape=[sds((NR, N, C), BF16), sds((5 * C, C), F32), sds((4, C, C), F32), sds((C, 128), F32), sds((C, 128), F32)],
        compiler_params=PARAMS,
        cost_estimate=COST,
        name="in_backward",
    )(ids, z_loc, dy_loc, m_loc, d_a, d_b, *dg_chunks, w_t, scale, offset, w_cat)


SHARD = 112
VECS = 6 * C
VEC_ROWS = (0, 1, 6, 7, 8, 9)


def sum_kernel(*refs):
    accs, wout_refs, osc_refs, bg_refs, w_ref = refs[:7], refs[7:11], refs[11:14], refs[14:17], refs[17]
    total, src, recv, mine, send1, recv1, send2, recv2 = refs[18:]
    me = lax.axis_index('dap')

    def peer(step):
        return {'dap': lax.rem(me + step, 8)}

    barrier = pltpu.get_barrier_semaphore()
    for step in range(1, 8):
        pl.semaphore_signal(barrier, inc=1, device_id=peer(step), device_id_type=pl.DeviceIdType.MESH)
    for blk in range(5):
        src[C * blk:C * (blk + 1)] = w_ref[C * blk:C * (blk + 1)].T
    src[5 * C:VECS] = sum(ref[...] for ref in wout_refs[1:]) + wout_refs[0][...]
    rows = []
    for ref, more in zip(accs, ((), (), (), osc_refs, (), (), bg_refs)):
        rows += [ref[n] for n in range(4)] if len(ref.shape) > 2 else [sum((other[...] for other in more), ref[...])]
    rows = [jnp.sum(val.T, axis=0, keepdims=True) for val in rows]
    src[VECS:] = jnp.concatenate(rows + [jnp.zeros((8 * SHARD - VECS - len(rows), C), F32)], axis=0)
    pl.semaphore_wait(barrier, 7)

    def shard(owner):
        return pl.ds(pl.multiple_of(owner * SHARD, 16), SHARD)

    copies = []
    for step in range(1, 8):
        copy = pltpu.make_async_remote_copy(
            src_ref=src.at[shard(lax.rem(me + step, 8))], dst_ref=recv.at[step], send_sem=send1.at[step], recv_sem=recv1.at[step],
            device_id=peer(step), device_id_type=pl.DeviceIdType.MESH)
        copy.start()
        copies.append(copy)
    val = src[shard(me), :]
    for step, copy in enumerate(copies):
        copy.wait()
        val += recv[step + 1]
    mine[...] = val.astype(BF16)
    total[shard(me), :] = val.astype(BF16)
    copies = []
    for step in range(1, 8):
        copy = pltpu.make_async_remote_copy(
            src_ref=mine, dst_ref=total.at[shard(me)], send_sem=send2.at[step], recv_sem=recv2.at[step],
            device_id=peer(step), device_id_type=pl.DeviceIdType.MESH)
        copy.start()
        copies.append(copy)
    for copy in copies:
        copy.wait()


def split_kernel(total, win_ref, wgate_ref, wout_ref, bin_ref, *vec_refs):
    for blk in range(4):
        win_ref[:, C * blk:C * (blk + 1)] = total[C * blk:C * (blk + 1)]
    wgate_ref[...] = total[4 * C:5 * C]
    wout_ref[...] = total[5 * C:VECS]
    vecs = total[VECS:VECS + 16]
    bin_ref[...] = vecs[2:6].reshape(4 * C)
    for ref, n in zip(vec_refs, VEC_ROWS):
        ref[...] = vecs[n:n + 1]


def vmem_specs(count):
    return [pl.BlockSpec(memory_space=pltpu.VMEM)] * count


def sum_call(accs, wouts, acc_w):
    args = [*accs, *wouts, acc_w]
    total = pl.pallas_call(
        sum_kernel,
        in_specs=vmem_specs(len(args)),
        out_specs=vmem_specs(1)[0],
        out_shape=sds((8 * SHARD, C), BF16),
        scratch_shapes=[pltpu.VMEM((8 * SHARD, C), F32), pltpu.VMEM((8, SHARD, C), F32), pltpu.VMEM((SHARD, C), BF16)]
        + [pltpu.SemaphoreType.DMA((8,))] * 4,
        compiler_params=pltpu.CompilerParams(collective_id=0, has_side_effects=True),
        cost_estimate=COST,
        name="sum_grads",
    )(*args)
    outs = [sds((C, width), BF16) for width in (4 * C, C, C)] + [sds((4 * C,), BF16)] + [sds((1, C), BF16)] * len(VEC_ROWS)
    return pl.pallas_call(
        split_kernel,
        in_specs=vmem_specs(1),
        out_specs=vmem_specs(len(outs)),
        out_shape=outs,
        cost_estimate=COST,
        name="split_grads",
    )(total)


def aug_weight(w_mat, bias):
    wide = jnp.zeros((w_mat.shape[1], 16), BF16).at[:, 0].set(bias)
    return jnp.concatenate([w_mat.T, wide], axis=1)


def column(vec, width):
    return jnp.broadcast_to(vec.astype(F32)[:, None], (C, width))


def local_grads(z_loc, mask_loc, dy_loc, ln_in_scale, ln_in_offset, w_in, b_in, ln_out_scale, ln_out_offset, w_out, b_out, w_gate, b_gate):
    me = lax.axis_index('dap')
    chip, core = me // 2, me % 2
    w_cat = jnp.concatenate([w_in, w_gate], axis=1)
    pa, pb, la, lb, gate = jnp.split(jnp.concatenate([w_cat, jnp.concatenate([b_in, b_gate])[None]], axis=0), 5, axis=1)
    w_t = jnp.concatenate([pa, la, pb, lb, gate], axis=1)
    w_t = aug_weight(w_t[:C], w_t[C])
    w_out_t = aug_weight(w_out, b_out)
    (in_scale, in_offset), wide_in = ((column(ln_in_scale, width), column(ln_in_offset, width)) for width in (WIDE, N))
    out_scale, out_offset = column(ln_out_scale, 128), column(ln_out_offset, 128)

    order = [((chip * 2) ^ HOPS[q][h]) * NR + core_of * NR + h * HALF for q in range(4) for core_of in range(2) for h in range(2)]
    ids = jnp.stack(order + [core]).astype(jnp.int32)
    mask_t = jnp.pad(mask_loc.T.astype(BF16), ((0, 0), (0, C - NR)))[None]

    def move(val, flips):
        return lax.ppermute(val, 'dap', [(d, d ^ flips) for d in range(8)])

    top, bottom = z_loc[:HALF], z_loc[HALF:]
    gathered = {}
    gathered[1, 0], gathered[1, 1] = move(top, HOPS[1][0]), move(bottom, HOPS[1][1])
    masks = {hop: move(mask_t, hop) for hop in (2, 4, 6)}
    gathered[2, 0], gathered[2, 1] = move(gathered[1, 0], HOPS[1][1]), move(gathered[1, 1], HOPS[1][0])
    gathered[3, 0], gathered[3, 1] = move(top, HOPS[3][0]), move(bottom, HOPS[3][1])

    a_own, b_own, dup, don, g1, acc_bout, acc_ooff, ids = own_call(ids, z_loc, dy_loc, mask_t, w_t, in_scale, in_offset, w_out)
    b_par, a_par = move(b_own, 1), move(a_own, 1)
    a_at = {(0, h, f): (val, h) for h in range(2) for f, val in ((0, a_own), (1, a_par))}
    b_at = {(0, h, f): (val, h) for h in range(2) for f, val in ((0, b_own), (1, b_par))}
    do_at, do_chunks, chunk_b, d_a, dg_chunks, sums = {}, [], [], [], [], []
    for q in range(4):
        for h in range(2):
            if q:
                act_a, act_b, ids = gated_call(h, ids, gathered[q, h], masks[HOPS[q][h]], w_t[:4 * C], in_scale, in_offset)
                a_at[q, h, 0], b_at[q, h, 0] = (act_a, 0), (act_b, 0)
                b_at[q, h, 1] = move(act_b, 1), 0
                a_at[q, h, 1] = move(act_a, 1), 0
        b_pieces = [b_at[q, h, f] for f in range(2) for h in range(2)]
        do_own, dg, same0, same1, cross0, cross1, *acc, ids = out_call(q, ids, a_own, b_pieces, don, dup, g1, w_out_t, out_scale, out_offset)
        do_chunks.append(do_own)
        dg_chunks.append(dg)
        sums.append(acc)
        chunk_b += b_pieces
        if q:
            d_a = da_call(do_chunks, chunk_b, d_a, BF16 if q == 3 else F32)
            do_chunks, chunk_b, d_a = [], [], [d_a]
        for flip, h, val in ((0, 0, same0), (0, 1, same1), (1, 0, cross0), (1, 1, cross1)):
            flips = HOPS[q][h] ^ flip
            do_at[h, flips] = move(val, flips) if flips else val
    chunk_of = {(HOPS[q][h], h): q for q in range(4) for h in range(2)}
    d_b = db_call([do_at[h, s] for h in range(2) for s in range(8)],
                  [a_at[chunk_of[s & 6, h], h, s & 1] for h in range(2) for s in range(8)])
    d_z, acc_w, acc_bin, acc_isc, acc_ioff = in_call(ids, z_loc, dy_loc, mask_t, d_a[0], d_b, dg_chunks, w_t[:4 * C], *wide_in, w_cat)

    wouts, oscs, bgs = zip(*sums)
    accs = (acc_isc, acc_ioff, acc_bin, oscs[0], acc_ooff, acc_bout, bgs[0])
    d_win, d_wgate, d_wout, *vecs = sum_call(accs, wouts + oscs[1:] + bgs[1:], acc_w)
    d_bin, d_isc, d_ioff, d_osc, d_ooff, d_bout, d_bg = (vec.reshape(vec.size) for vec in vecs)
    return d_z, d_isc, d_ioff, d_win, d_bin, d_osc, d_ooff, d_wout, d_bout, d_wgate, d_bg


def solution(mesh):
    pair_spec = P(('batch', 'dap'), None, None)
    mask_spec = P(('batch', 'dap'), None)
    vec_rep = P(None)
    mat_rep = P(None, None)
    vec_part = P('batch')
    mat_part = P('batch', None)
    in_specs = (pair_spec, mask_spec, pair_spec, vec_rep, vec_rep, mat_rep, vec_rep, vec_rep, vec_rep, mat_rep, vec_rep, mat_rep, vec_rep)
    out_specs = (pair_spec, vec_part, vec_part, mat_part, vec_part, vec_part, vec_part, mat_part, vec_part, mat_part, vec_part)
    return jax.shard_map(local_grads, mesh=mesh, in_specs=in_specs, out_specs=out_specs, check_vma=False)
```

```python
import functools
import jax
import jax.numpy as jnp
from jax import lax
from jax.experimental import pallas as pl
from jax.experimental.pallas import tpu as pltpu
from jax.sharding import PartitionSpec as P

LN_EPS = 1e-5
N = 512
C = 128
NR = 64
NB = 16
NQ = NR // NB
HALF = NR // 2
HOPS = ((0, 0), (2, 4), (6, 6), (4, 2))
SB = NB + 4
SO = NR + 4
WIDE = N // 2
F32 = jnp.float32
BF16 = jnp.bfloat16
PARAMS = pltpu.CompilerParams(vmem_limit_bytes=60 << 20)
COST = pl.CostEstimate(flops=1 << 33, bytes_accessed=1 << 26, transcendentals=0)


def sds(shape, dtype):
    return jax.ShapeDtypeStruct(shape, dtype)


def full_spec(shape):
    return pl.BlockSpec(shape, lambda *ids: (0,) * len(shape))


def sigmoid(x_val):
    return 1.0 / (1.0 + jnp.exp(-x_val))


def nt_dot(lhs, rhs):
    return lax.dot_general(lhs, rhs, (((1,), (1,)), ((), ())), preferred_element_type=F32)


def nn_dot(lhs, rhs):
    return lax.dot_general(lhs, rhs, (((1,), (0,)), ((), ())), preferred_element_type=F32)


def ones_rows(width):
    return jnp.where(lax.broadcasted_iota(jnp.int32, (16, width), 0) == 0, 1.0, 0.0).astype(BF16)


def norm_rows(x_val):
    mean_val = jnp.mean(x_val, axis=0, keepdims=True)
    centered = x_val - mean_val
    inv_std = lax.rsqrt(jnp.mean(centered * centered, axis=0, keepdims=True) + LN_EPS)
    return centered * inv_std, inv_std


def put_row(scr, row, pitch, val, lane=0):
    for tile in jnp.split(val, val.shape[1] // C, axis=1):
        scr[lane, pl.ds(row, C, stride=pitch), :] = tile
        lane += 1


def get_row(scr, row, pitch, lanes):
    return jnp.concatenate([scr[lane, pl.ds(row, C, stride=pitch), :] for lane in lanes], axis=1)


def flush_rows(scr, out_ref):
    def body(ch, carry):
        for lane in range(4):
            out_ref[ch, :, C * lane:C * (lane + 1)] = scr[lane, pl.ds(ch * SB, NB), :].astype(BF16)
        return carry

    lax.fori_loop(0, C, body, 0, unroll=8)


def gated_half(w_ref, scrs, row, half, z_norm, mask_f):
    aug = jnp.concatenate([z_norm, ones_rows(WIDE)], axis=0)
    for side, scr in enumerate(scrs):
        proj = nn_dot(w_ref[2 * C * side:2 * C * (side + 1)], aug)
        put_row(scr, row, SB, mask_f * sigmoid(proj[C:]) * proj[:C], 2 * half)
    return aug


def halves():
    return ((half, slice(WIDE * half, WIDE * (half + 1))) for half in range(2))


def pair_row(ref, row, ids_ref, half):
    return jnp.concatenate([ref[row, pl.ds(pl.multiple_of(ids_ref[8 * half + p], HALF), HALF), :] for p in range(8)], axis=0)


def normed_row(z_row, scale, offset):
    z_t = z_row.T.astype(F32)
    x_hat, inv_std = norm_rows(z_t)
    z_norm = (x_hat * scale + offset).astype(BF16)
    return x_hat, inv_std, z_norm


def pass_ids(ids_ref, tok_ref):
    for p in range(17):
        tok_ref[p] = ids_ref[p]


TOKEN = sds((17,), jnp.int32)
TOKEN_SPEC = pl.BlockSpec(memory_space=pltpu.SMEM)


def load_mask(m_ref, m_scr, t_scr, ids_ref):
    t_scr[...] = m_ref[...].astype(F32).T
    for half, cols in halves():
        m_scr[:, cols] = jnp.concatenate([t_scr[pl.ds(pl.multiple_of(ids_ref[8 * half + p], HALF), HALF), :] for p in range(8)], axis=0).T


def gated_kernel(half_id, ids_ref, z_ref, m_ref, w_ref, scale_ref, offset_ref, a_ref, b_ref, tok_ref, a_scr, b_scr, m_scr, t_scr):
    pass_ids(ids_ref, tok_ref)
    load_mask(m_ref, m_scr, t_scr, ids_ref)
    first = half_id * HALF + pl.program_id(0) * NB

    def body(row, carry):
        for half, cols in halves():
            _, _, z_norm = normed_row(pair_row(z_ref, row, ids_ref, half), scale_ref[...], offset_ref[...])
            gated_half(w_ref, (a_scr, b_scr), row, half, z_norm, m_scr[pl.ds(first + row, 1), cols])
        return carry

    lax.fori_loop(0, NB, body, 0, unroll=8)
    flush_rows(a_scr, a_ref)
    flush_rows(b_scr, b_ref)


def gated_call(half_id, ids, piece, mask_t, w_t, scale, offset):
    out_spec = pl.BlockSpec((C, NB, N), lambda r, ids: (0, r, 0))
    return pl.pallas_call(
        functools.partial(gated_kernel, half_id),
        grid_spec=pltpu.PrefetchScalarGridSpec(
            num_scalar_prefetch=1,
            grid=(HALF // NB,),
            in_specs=[
                pl.BlockSpec((NB, N, C), lambda r, ids: (r, 0, 0)),
                full_spec((NR, N)),
                full_spec((4 * C, C + 16)), full_spec((C, WIDE)), full_spec((C, WIDE)),
            ],
            out_specs=[out_spec, out_spec, TOKEN_SPEC],
            scratch_shapes=[pltpu.VMEM((4, C * SB, 128), F32)] * 2 + [pltpu.VMEM((NR, N), F32), pltpu.VMEM((N, NR), F32)],
        ),
        out_shape=[sds((C, HALF, N), BF16)] * 2 + [TOKEN],
        compiler_params=PARAMS,
        cost_estimate=COST,
        name="gated_rows",
    )(ids, piece, mask_t, w_t, scale, offset)


def lanes(val):
    half = val.shape[1] // 2
    return val[:, :half] + val[:, half:]


def own_kernel(ids_ref, z_ref, dy_ref, m_ref, w_ref, scale_ref, offset_ref, w_out_ref,
               a_ref, b_ref, dup_ref, don_ref, g1_ref, dbout_ref, dooff_ref, tok_ref, a_scr, b_scr, m_scr, t_scr):
    pass_ids(ids_ref, tok_ref)

    @pl.when(pl.program_id(0) == 0)
    def _():
        dbout_ref[...] = jnp.zeros_like(dbout_ref)
        dooff_ref[...] = jnp.zeros_like(dooff_ref)

    load_mask(m_ref, m_scr, t_scr, ids_ref)
    first = pl.program_id(0) * NB

    def body(row, carry):
        for half, cols in halves():
            _, _, z_norm = normed_row(pair_row(z_ref, row, ids_ref, half), scale_ref[...], offset_ref[...])
            aug = gated_half(w_ref, (a_scr, b_scr), row, half, z_norm, m_scr[pl.ds(first + row, 1), cols])
            sig_g = sigmoid(nn_dot(w_ref[4 * C:5 * C], aug))
            d_upd = sig_g * pair_row(dy_ref, row, ids_ref, half).T.astype(F32)
            g1_ref[row, :, cols] = d_upd * (1.0 - sig_g)
            d_upd16 = d_upd.astype(BF16)
            dup_ref[row, :, cols] = d_upd16
            d_onorm = nn_dot(w_out_ref[...], d_upd16).astype(BF16)
            don_ref[row, :, cols] = d_onorm
            dbout_ref[...] += lanes(d_upd16.astype(F32))
            dooff_ref[...] += lanes(d_onorm.astype(F32))
        return carry

    lax.fori_loop(0, NB, body, 0, unroll=4)
    flush_rows(a_scr, a_ref)
    flush_rows(b_scr, b_ref)


def own_call(ids, z_loc, dy_loc, m_loc, w_t, scale, offset, w_out):
    row_spec = pl.BlockSpec((NB, N, C), lambda r, ids: (r, 0, 0))
    t_spec = pl.BlockSpec((NB, C, N), lambda r, ids: (r, 0, 0))
    act_spec = pl.BlockSpec((C, NB, N), lambda r, ids: (0, r, 0))
    return pl.pallas_call(
        own_kernel,
        grid_spec=pltpu.PrefetchScalarGridSpec(
            num_scalar_prefetch=1,
            grid=(NQ,),
            in_specs=[row_spec, row_spec, full_spec((NR, N)),
                      full_spec((5 * C, C + 16)), full_spec((C, WIDE)), full_spec((C, WIDE)), full_spec((C, C))],
            out_specs=[act_spec, act_spec, t_spec, t_spec, t_spec, full_spec((C, 128)), full_spec((C, 128)), TOKEN_SPEC],
            scratch_shapes=[pltpu.VMEM((4, C * SB, 128), F32)] * 2 + [pltpu.VMEM((NR, N), F32), pltpu.VMEM((N, NR), F32)],
        ),
        out_shape=[sds((C, NR, N), BF16), sds((C, NR, N), BF16), sds((NR, C, N), BF16), sds((NR, C, N), BF16), sds((NR, C, N), F32), sds((C, 128), F32), sds((C, 128), F32), TOKEN],
        compiler_params=PARAMS,
        cost_estimate=COST,
        name="own_rows",
    )(ids, z_loc, dy_loc, m_loc, w_t, scale, offset, w_out)


CB = 32
CR = 32
CP = 64
FIRST = C // CB
LAST = FIRST + NR // CR


def out_kernel(ids_ref, a_ref, b_own0, b_own1, b_par0, b_par1, don_ref, dup_ref, g1_ref, w_out_ref, scale_ref, offset_ref,
               do_ref, dg_ref, *rest):
    dwout_ref, dosc_ref, dbg_ref, tok_ref, o_scr = rest[-5:]
    same0, same1, cross0, cross1 = rest[:-5] if len(rest) > 7 else [ref.at[h] for ref in rest[:2] for h in range(2)]
    step = pl.program_id(0)
    first_core = ids_ref[16] == 0

    @pl.when(step == 0)
    def _():
        pass_ids(ids_ref, tok_ref)
        dwout_ref[...] = jnp.zeros_like(dwout_ref)
        dosc_ref[...] = jnp.zeros_like(dosc_ref)
        dbg_ref[...] = jnp.zeros_like(dbg_ref)

    @pl.when(step < FIRST)
    def _():
        def prod(ch, carry):
            b_rows = jnp.concatenate([ref[ch] for ref in (b_own0, b_own1, b_par0, b_par1)], axis=0)
            val = nt_dot(a_ref[ch], b_rows)
            o_scr[0, pl.ds((step * CB + ch) * SO, NR), :] = jnp.where(first_core, val, pltpu.roll(val, 64, 1))
            return carry

        lax.fori_loop(0, CB, prod, 0, unroll=16)

    @pl.when((step >= FIRST) & (step < LAST))
    def _():
        def chain(row, carry):
            o_row = (step - FIRST) * CR + row
            o_hat, inv_std = norm_rows(get_row(o_scr, o_row, SO, (0,)))
            o_norm = (o_hat * scale_ref[...] + offset_ref[...]).astype(BF16)
            aug = jnp.concatenate([o_norm, ones_rows(C)], axis=0)
            upd = nn_dot(w_out_ref[...], aug).astype(BF16).astype(F32)
            d_gate = g1_ref[row] * upd
            dbg_ref[...] += d_gate
            dg_ref[row] = d_gate.astype(BF16)
            d_onorm = don_ref[row].astype(F32)
            dosc_ref[...] += d_onorm * o_hat
            grad_hat = d_onorm * scale_ref[...]
            mean_grad = jnp.mean(grad_hat, axis=0, keepdims=True)
            mean_proj = jnp.mean(grad_hat * o_hat, axis=0, keepdims=True)
            put_row(o_scr, o_row, SO, inv_std * (grad_hat - mean_grad - o_hat * mean_proj))
            dwout_ref[...] += nt_dot(o_norm, dup_ref[row])
            return carry

        lax.fori_loop(0, CR, chain, 0, unroll=8)

    @pl.when(step >= LAST)
    def _():
        lane = lax.broadcasted_iota(jnp.int32, (NB, C), 1)
        low = lane < 64
        even = lane % 64 < HALF

        def swap(left, right, keep, width):
            return jnp.where(keep, left, pltpu.roll(right, width, 1)), jnp.where(keep, pltpu.roll(left, C - width, 1), right)

        def pack(ch, carry):
            val = o_scr[0, pl.ds(((step - LAST) * CP + ch) * SO, NR), :]
            do_ref[ch] = jnp.where(first_core, val, pltpu.roll(val, 64, 1)).astype(BF16)
            g0, g1, g2, g3 = jnp.split(val, 4, axis=0)
            g0, g2 = swap(g0, g2, low, 64)
            g1, g3 = swap(g1, g3, low, 64)
            g0, g1 = swap(g0, g1, even, HALF)
            g2, g3 = swap(g2, g3, even, HALF)
            same0[ch] = jnp.where(first_core, g0, g2).astype(BF16)
            same1[ch] = jnp.where(first_core, g1, g3).astype(BF16)
            cross0[ch] = jnp.where(first_core, g2, g0).astype(BF16)
            cross1[ch] = jnp.where(first_core, g3, g1).astype(BF16)
            return carry

        lax.fori_loop(0, CP, pack, 0, unroll=8)


def piece_spec(width, blk):
    return pl.BlockSpec((width, HALF, N), lambda s, *ids: (s, blk, 0))


def prod_step(step):
    return jnp.minimum(step, FIRST - 1)


def chain_step(step):
    return jnp.clip(step - FIRST, 0, NR // CR - 1)


def pack_step(step):
    return jnp.clip(step - LAST, 0, C // CP - 1)


def out_call(chunk, ids, a_own, b_pieces, don, dup, g1, w_out_t, scale, offset):
    lane_spec = pl.BlockSpec((CR, C, C), lambda s, ids: (chain_step(s), 0, chunk))
    acc_spec = full_spec((C, C))
    if chunk % 2:
        packs, pack_spec = [sds((C, NB, C), BF16)] * 4, pl.BlockSpec((CP, NB, C), lambda s, ids: (pack_step(s), 0, 0))
    else:
        packs, pack_spec = [sds((2, C, NB, C), BF16)] * 2, pl.BlockSpec((2, CP, NB, C), lambda s, ids: (0, pack_step(s), 0, 0))
    b_specs = [pl.BlockSpec((CB, HALF, N), lambda s, ids, blk=blk: (prod_step(s), blk, 0)) for _, blk in b_pieces]
    return pl.pallas_call(
        out_kernel,
        grid_spec=pltpu.PrefetchScalarGridSpec(
            num_scalar_prefetch=1,
            grid=(LAST + C // CP,),
            in_specs=[pl.BlockSpec((CB, NR, N), lambda s, ids: (prod_step(s), 0, 0))] + b_specs
            + [lane_spec, lane_spec, lane_spec, full_spec((C, C + 16)), acc_spec, acc_spec],
            out_specs=[pl.BlockSpec((CP, NR, C), lambda s, ids: (pack_step(s), 0, 0)),
                       pl.BlockSpec((CR, C, C), lambda s, ids: (chain_step(s), 0, 0))] + [pack_spec] * len(packs) + [acc_spec] * 3 + [TOKEN_SPEC],
            scratch_shapes=[pltpu.VMEM((1, C * SO, C), F32)],
        ),
        out_shape=[sds((C, NR, C), BF16), sds((NR, C, C), BF16)] + packs + [sds((C, C), F32)] * 3 + [TOKEN],
        compiler_params=PARAMS,
        cost_estimate=COST,
        name="out_chain",
    )(ids, a_own, *(arr for arr, _ in b_pieces), don, dup, g1, w_out_t, scale, offset)


CK = 16


def da_kernel(count, *refs):
    do_refs, b_refs, da_ref = refs[:count], refs[count:5 * count], refs[-1]
    for ch in range(CK):
        do_row = jnp.concatenate([ref[ch] for ref in do_refs], axis=1)
        b_rows = jnp.concatenate([ref[ch] for ref in b_refs], axis=0)
        val = nn_dot(do_row, b_rows)
        for ref in refs[5 * count:-1]:
            val += ref[ch]
        da_ref[ch] = val.astype(da_ref.dtype)


def da_call(do_chunks, b_pieces, partial, dtype):
    row_spec = pl.BlockSpec((CK, NR, N), lambda s: (s, 0, 0))
    return pl.pallas_call(
        functools.partial(da_kernel, len(do_chunks)),
        grid=(C // CK,),
        in_specs=[pl.BlockSpec((CK, NR, C), lambda s: (s, 0, 0))] * len(do_chunks) + [piece_spec(CK, blk) for _, blk in b_pieces] + [row_spec] * len(partial),
        out_specs=row_spec,
        out_shape=sds((C, NR, N), dtype),
        compiler_params=PARAMS,
        cost_estimate=COST,
        name="grad_a",
    )(*do_chunks, *(arr for arr, _ in b_pieces), *partial)


def db_kernel(*refs):
    do_refs, a_refs, db_ref = refs[:16], refs[16:32], refs[32]
    for ch in range(CK):
        x_t = [jnp.concatenate([ref[ch] for ref in do_refs[8 * h:8 * h + 8]], axis=0).T for h in range(2)]
        total = None
        for g in range(4):
            lhs = jnp.concatenate([x[32 * g:32 * g + 32] for x in x_t], axis=0)
            half, sub = divmod(g, 2)
            rhs = jnp.concatenate([ref[ch, NB * sub:NB * (sub + 1), :] for ref in a_refs[8 * half:8 * half + 8]], axis=0)
            term = nn_dot(lhs, rhs)
            total = term if total is None else total + term
        db_ref[ch] = total.astype(BF16)


def do_spec(arr, half):
    if len(arr.shape) > 3:
        return pl.BlockSpec((None, CK, NB, C), lambda s: (half, s, 0, 0))
    return pl.BlockSpec((CK, NB, C), lambda s: (s, 0, 0))


def db_call(do_pieces, a_pieces):
    return pl.pallas_call(
        db_kernel,
        grid=(C // CK,),
        in_specs=[do_spec(*piece) for piece in do_pieces] + [piece_spec(CK, blk) for _, blk in a_pieces],
        out_specs=pl.BlockSpec((CK, NR, N), lambda s: (s, 0, 0)),
        out_shape=sds((C, NR, N), BF16),
        compiler_params=PARAMS,
        cost_estimate=COST,
        name="grad_b",
    )(*(arr for arr, _ in do_pieces), *(arr for arr, _ in a_pieces))


def in_kernel(ids_ref, z_ref, dy_ref, m_ref, da_ref, db_ref, dg0, dg1, dg2, dg3, w_ref, scale_ref, offset_ref, w_cat_ref,
              dz_ref, dw_ref, dbin_ref, dsc_ref, doff_ref, a_scr, b_scr, m_scr, t_scr):
    dgs = (dg0, dg1, dg2, dg3)

    @pl.when(pl.program_id(0) == 0)
    def _():
        dw_ref[...] = jnp.zeros_like(dw_ref)
        dbin_ref[...] = jnp.zeros_like(dbin_ref)
        dsc_ref[...] = jnp.zeros_like(dsc_ref)
        doff_ref[...] = jnp.zeros_like(doff_ref)

    def unpack(ch, carry):
        for src, scr in ((da_ref, a_scr), (db_ref, b_scr)):
            for lane in range(4):
                scr[lane, pl.ds(ch * SB, NB), :] = src[ch, :, C * lane:C * (lane + 1)].astype(F32)
        return carry

    lax.fori_loop(0, C, unpack, 0, unroll=4)

    load_mask(m_ref, m_scr, t_scr, ids_ref)
    first = pl.program_id(0) * NB

    def lanes4(val):
        return lanes(lanes(val))

    def body(row, carry):
        def full_row(ref):
            return jnp.concatenate([pair_row(ref, row, ids_ref, half) for half in range(2)], axis=0)

        x_hat, inv_std, z_norm = normed_row(full_row(z_ref), scale_ref[...], offset_ref[...])
        aug = jnp.concatenate([z_norm, ones_rows(N)], axis=0)
        mask_f = m_scr[pl.ds(first + row, 1), :]
        parts = []
        for side, scr in ((0, a_scr), (1, b_scr)):
            proj = nn_dot(w_ref[2 * C * side:2 * C * (side + 1)], aug)
            sig = sigmoid(proj[C:])
            d_proj = get_row(scr, row, SB, range(4)) * mask_f * sig
            d_lin = d_proj * proj[:C] * (1.0 - sig)
            dbin_ref[side] += lanes4(d_proj)
            dbin_ref[2 + side] += lanes4(d_lin)
            parts.append((d_proj.astype(BF16), d_lin.astype(BF16)))
        d_gate = jnp.concatenate([dg[row] for dg in dgs], axis=1)
        cat = jnp.concatenate([part[kind] for kind in range(2) for part in parts] + [d_gate], axis=0)
        dw_ref[...] += nt_dot(cat, z_norm)
        d_znorm = nn_dot(w_cat_ref[...], cat).astype(BF16).astype(F32)
        dsc_ref[...] += lanes4(d_znorm * x_hat)
        doff_ref[...] += lanes4(d_znorm)
        grad_hat = d_znorm * scale_ref[...]
        mean_grad = jnp.mean(grad_hat, axis=0, keepdims=True)
        mean_proj = jnp.mean(grad_hat * x_hat, axis=0, keepdims=True)
        d_zt = inv_std * (grad_hat - mean_grad - x_hat * mean_proj)
        d_row = (full_row(dy_ref).astype(F32) + d_zt.T).astype(BF16)
        for p in range(16):
            dz_ref[row, pl.ds(pl.multiple_of(ids_ref[p], HALF), HALF), :] = d_row[HALF * p:HALF * (p + 1)]
        return carry

    lax.fori_loop(0, NB, body, 0, unroll=8)


def in_call(ids, z_loc, dy_loc, m_loc, d_a, d_b, dg_chunks, w_t, scale, offset, w_cat):
    row_spec = pl.BlockSpec((NB, N, C), lambda r, ids: (r, 0, 0))
    act_spec = pl.BlockSpec((C, NB, N), lambda r, ids: (0, r, 0))
    return pl.pallas_call(
        in_kernel,
        grid_spec=pltpu.PrefetchScalarGridSpec(
            num_scalar_prefetch=1,
            grid=(NQ,),
            in_specs=[row_spec, row_spec, full_spec((NR, N)), act_spec, act_spec]
            + [pl.BlockSpec((NB, C, 128), lambda r, ids: (r, 0, 0))] * 4
            + [full_spec((4 * C, C + 16)), full_spec((C, N)), full_spec((C, N)), full_spec((C, 5 * C))],
            out_specs=[row_spec, full_spec((5 * C, C)), full_spec((4, C, C)), full_spec((C, 128)), full_spec((C, 128))],
            scratch_shapes=[pltpu.VMEM((4, C * SB, 128), F32)] * 2 + [pltpu.VMEM((NR, N), F32), pltpu.VMEM((N, NR), F32)],
        ),
        out_shape=[sds((NR, N, C), BF16), sds((5 * C, C), F32), sds((4, C, C), F32), sds((C, 128), F32), sds((C, 128), F32)],
        compiler_params=PARAMS,
        cost_estimate=COST,
        name="in_backward",
    )(ids, z_loc, dy_loc, m_loc, d_a, d_b, *dg_chunks, w_t, scale, offset, w_cat)


SHARD = 112
VECS = 6 * C
VEC_ROWS = (0, 1, 6, 7, 8, 9)


def sum_kernel(*refs):
    accs, wout_refs, osc_refs, bg_refs, w_ref = refs[:7], refs[7:11], refs[11:14], refs[14:17], refs[17]
    total, src, recv, mine, send1, recv1, send2, recv2 = refs[18:]
    me = lax.axis_index('dap')

    def peer(step):
        return {'dap': lax.rem(me + step, 8)}

    barrier = pltpu.get_barrier_semaphore()
    for step in range(1, 8):
        pl.semaphore_signal(barrier, inc=1, device_id=peer(step), device_id_type=pl.DeviceIdType.MESH)
    for blk in range(5):
        src[C * blk:C * (blk + 1)] = w_ref[C * blk:C * (blk + 1)].T
    src[5 * C:VECS] = sum(ref[...] for ref in wout_refs[1:]) + wout_refs[0][...]
    rows = []
    for ref, more in zip(accs, ((), (), (), osc_refs, (), (), bg_refs)):
        rows += [ref[n] for n in range(4)] if len(ref.shape) > 2 else [sum((other[...] for other in more), ref[...])]
    rows = [jnp.sum(val.T, axis=0, keepdims=True) for val in rows]
    src[VECS:] = jnp.concatenate(rows + [jnp.zeros((8 * SHARD - VECS - len(rows), C), F32)], axis=0)
    pl.semaphore_wait(barrier, 7)

    def shard(owner):
        return pl.ds(pl.multiple_of(owner * SHARD, 16), SHARD)

    copies = []
    for step in range(1, 8):
        copy = pltpu.make_async_remote_copy(
            src_ref=src.at[shard(lax.rem(me + step, 8))], dst_ref=recv.at[step], send_sem=send1.at[step], recv_sem=recv1.at[step],
            device_id=peer(step), device_id_type=pl.DeviceIdType.MESH)
        copy.start()
        copies.append(copy)
    val = src[shard(me), :]
    for step, copy in enumerate(copies):
        copy.wait()
        val += recv[step + 1]
    mine[...] = val.astype(BF16)
    total[shard(me), :] = val.astype(BF16)
    copies = []
    for step in range(1, 8):
        copy = pltpu.make_async_remote_copy(
            src_ref=mine, dst_ref=total.at[shard(me)], send_sem=send2.at[step], recv_sem=recv2.at[step],
            device_id=peer(step), device_id_type=pl.DeviceIdType.MESH)
        copy.start()
        copies.append(copy)
    for copy in copies:
        copy.wait()


def split_kernel(total, win_ref, wgate_ref, wout_ref, bin_ref, *vec_refs):
    for blk in range(4):
        win_ref[:, C * blk:C * (blk + 1)] = total[C * blk:C * (blk + 1)]
    wgate_ref[...] = total[4 * C:5 * C]
    wout_ref[...] = total[5 * C:VECS]
    vecs = total[VECS:VECS + 16]
    bin_ref[...] = vecs[2:6].reshape(4 * C)
    for ref, n in zip(vec_refs, VEC_ROWS):
        ref[...] = vecs[n:n + 1]


def vmem_specs(count):
    return [pl.BlockSpec(memory_space=pltpu.VMEM)] * count


def sum_call(accs, wouts, acc_w):
    args = [*accs, *wouts, acc_w]
    total = pl.pallas_call(
        sum_kernel,
        in_specs=vmem_specs(len(args)),
        out_specs=vmem_specs(1)[0],
        out_shape=sds((8 * SHARD, C), BF16),
        scratch_shapes=[pltpu.VMEM((8 * SHARD, C), F32), pltpu.VMEM((8, SHARD, C), F32), pltpu.VMEM((SHARD, C), BF16)]
        + [pltpu.SemaphoreType.DMA((8,))] * 4,
        compiler_params=pltpu.CompilerParams(collective_id=0, has_side_effects=True),
        cost_estimate=COST,
        name="sum_grads",
    )(*args)
    outs = [sds((C, width), BF16) for width in (4 * C, C, C)] + [sds((4 * C,), BF16)] + [sds((1, C), BF16)] * len(VEC_ROWS)
    return pl.pallas_call(
        split_kernel,
        in_specs=vmem_specs(1),
        out_specs=vmem_specs(len(outs)),
        out_shape=outs,
        cost_estimate=COST,
        name="split_grads",
    )(total)


def aug_weight(w_mat, bias):
    wide = jnp.zeros((w_mat.shape[1], 16), BF16).at[:, 0].set(bias)
    return jnp.concatenate([w_mat.T, wide], axis=1)


def column(vec, width):
    return jnp.broadcast_to(vec.astype(F32)[:, None], (C, width))


def local_grads(z_loc, mask_loc, dy_loc, ln_in_scale, ln_in_offset, w_in, b_in, ln_out_scale, ln_out_offset, w_out, b_out, w_gate, b_gate):
    me = lax.axis_index('dap')
    chip, core = me // 2, me % 2
    w_cat = jnp.concatenate([w_in, w_gate], axis=1)
    pa, pb, la, lb, gate = jnp.split(jnp.concatenate([w_cat, jnp.concatenate([b_in, b_gate])[None]], axis=0), 5, axis=1)
    w_t = jnp.concatenate([pa, la, pb, lb, gate], axis=1)
    w_t = aug_weight(w_t[:C], w_t[C])
    w_out_t = aug_weight(w_out, b_out)
    (in_scale, in_offset), wide_in = ((column(ln_in_scale, width), column(ln_in_offset, width)) for width in (WIDE, N))
    out_scale, out_offset = column(ln_out_scale, 128), column(ln_out_offset, 128)

    order = [((chip * 2) ^ HOPS[q][h]) * NR + core_of * NR + h * HALF for q in range(4) for core_of in range(2) for h in range(2)]
    ids = jnp.stack(order + [core]).astype(jnp.int32)
    mask_t = mask_loc.astype(BF16)

    def move(val, flips):
        return lax.ppermute(val, 'dap', [(d, d ^ flips) for d in range(8)])

    top, bottom = z_loc[:HALF], z_loc[HALF:]
    gathered = {}
    gathered[1, 0], gathered[1, 1] = move(top, HOPS[1][0]), move(bottom, HOPS[1][1])
    masks = {hop: move(mask_t, hop) for hop in (2, 4, 6)}
    gathered[2, 0], gathered[2, 1] = move(gathered[1, 0], HOPS[1][1]), move(gathered[1, 1], HOPS[1][0])
    gathered[3, 0], gathered[3, 1] = move(top, HOPS[3][0]), move(bottom, HOPS[3][1])

    a_own, b_own, dup, don, g1, acc_bout, acc_ooff, ids = own_call(ids, z_loc, dy_loc, mask_t, w_t, in_scale, in_offset, w_out)
    b_par, a_par = move(b_own, 1), move(a_own, 1)
    a_at = {(0, h, f): (val, h) for h in range(2) for f, val in ((0, a_own), (1, a_par))}
    b_at = {(0, h, f): (val, h) for h in range(2) for f, val in ((0, b_own), (1, b_par))}
    do_at, do_chunks, chunk_b, d_a, dg_chunks, sums = {}, [], [], [], [], []
    for q in range(4):
        for h in range(2):
            if q:
                act_a, act_b, ids = gated_call(h, ids, gathered[q, h], masks[HOPS[q][h]], w_t[:4 * C], in_scale, in_offset)
                a_at[q, h, 0], b_at[q, h, 0] = (act_a, 0), (act_b, 0)
                b_at[q, h, 1] = move(act_b, 1), 0
                a_at[q, h, 1] = move(act_a, 1), 0
        b_pieces = [b_at[q, h, f] for f in range(2) for h in range(2)]
        do_own, dg, *packs, acc_out, acc_osc, acc_bg, ids = out_call(q, ids, a_own, b_pieces, don, dup, g1, w_out_t, out_scale, out_offset)
        do_chunks.append(do_own)
        dg_chunks.append(dg)
        sums.append((acc_out, acc_osc, acc_bg))
        chunk_b += b_pieces
        if q:
            d_a = da_call(do_chunks, chunk_b, d_a, BF16 if q == 3 else F32)
            do_chunks, chunk_b, d_a = [], [], [d_a]
        for n, val in enumerate(packs):
            flip, h = divmod(n, 2) if q % 2 else (n, 0)
            flips = HOPS[q][h] ^ flip
            val = move(val, flips) if flips else val
            if q % 2:
                do_at[h, flips] = (val, h)
            else:
                do_at[0, flips], do_at[1, flips] = (val, 0), (val, 1)
    chunk_of = {(HOPS[q][h], h): q for q in range(4) for h in range(2)}
    d_b = db_call([do_at[h, s] for h in range(2) for s in range(8)],
                  [a_at[chunk_of[s & 6, h], h, s & 1] for h in range(2) for s in range(8)])
    d_z, acc_w, acc_bin, acc_isc, acc_ioff = in_call(ids, z_loc, dy_loc, mask_t, d_a[0], d_b, dg_chunks, w_t[:4 * C], *wide_in, w_cat)

    wouts, oscs, bgs = zip(*sums)
    accs = (acc_isc, acc_ioff, acc_bin, oscs[0], acc_ooff, acc_bout, bgs[0])
    d_win, d_wgate, d_wout, *vecs = sum_call(accs, wouts + oscs[1:] + bgs[1:], acc_w)
    d_bin, d_isc, d_ioff, d_osc, d_ooff, d_bout, d_bg = (vec.reshape(vec.size) for vec in vecs)
    return d_z, d_isc, d_ioff, d_win, d_bin, d_osc, d_ooff, d_wout, d_bout, d_wgate, d_bg


def solution(mesh):
    pair_spec = P(('batch', 'dap'), None, None)
    mask_spec = P(('batch', 'dap'), None)
    vec_rep = P(None)
    mat_rep = P(None, None)
    vec_part = P('batch')
    mat_part = P('batch', None)
    in_specs = (pair_spec, mask_spec, pair_spec, vec_rep, vec_rep, mat_rep, vec_rep, vec_rep, vec_rep, mat_rep, vec_rep, mat_rep, vec_rep)
    out_specs = (pair_spec, vec_part, vec_part, mat_part, vec_part, vec_part, vec_part, mat_part, vec_part, mat_part, vec_part)
    return jax.shard_map(local_grads, mesh=mesh, in_specs=in_specs, out_specs=out_specs, check_vma=False)
```

```python
import functools
import jax
import jax.numpy as jnp
from jax import lax
from jax.experimental import pallas as pl
from jax.experimental.pallas import tpu as pltpu
from jax.sharding import PartitionSpec as P

LN_EPS = 1e-5
N = 512
C = 128
NR = 64
NB = 16
NQ = NR // NB
HALF = NR // 2
HOPS = ((0, 0), (2, 4), (6, 6), (4, 2))
SB = NB + 4
SO = NR + 4
WIDE = N // 2
F32 = jnp.float32
BF16 = jnp.bfloat16
PARAMS = pltpu.CompilerParams(vmem_limit_bytes=60 << 20)
COST = pl.CostEstimate(flops=1 << 33, bytes_accessed=1 << 26, transcendentals=0)


def sds(shape, dtype):
    return jax.ShapeDtypeStruct(shape, dtype)


def full_spec(shape):
    return pl.BlockSpec(shape, lambda *ids: (0,) * len(shape))


def sigmoid(x_val):
    return 1.0 / (1.0 + jnp.exp(-x_val))


def nt_dot(lhs, rhs):
    return lax.dot_general(lhs, rhs, (((1,), (1,)), ((), ())), preferred_element_type=F32)


def nn_dot(lhs, rhs):
    return lax.dot_general(lhs, rhs, (((1,), (0,)), ((), ())), preferred_element_type=F32)


def ones_rows(width):
    return jnp.where(lax.broadcasted_iota(jnp.int32, (16, width), 0) == 0, 1.0, 0.0).astype(BF16)


def norm_rows(x_val):
    mean_val = jnp.mean(x_val, axis=0, keepdims=True)
    centered = x_val - mean_val
    inv_std = lax.rsqrt(jnp.mean(centered * centered, axis=0, keepdims=True) + LN_EPS)
    return centered * inv_std, inv_std


def put_row(scr, row, pitch, val, lane=0):
    for tile in jnp.split(val, val.shape[1] // C, axis=1):
        scr[lane, pl.ds(row, C, stride=pitch), :] = tile
        lane += 1


def get_row(scr, row, pitch, lanes):
    return jnp.concatenate([scr[lane, pl.ds(row, C, stride=pitch), :] for lane in lanes], axis=1)


def flush_rows(scr, out_ref):
    def body(ch, carry):
        for lane in range(4):
            out_ref[ch, :, C * lane:C * (lane + 1)] = scr[lane, pl.ds(ch * SB, NB), :].astype(BF16)
        return carry

    lax.fori_loop(0, C, body, 0, unroll=8)


def gated_half(w_ref, scrs, row, half, z_norm, mask_f):
    aug = jnp.concatenate([z_norm, ones_rows(WIDE)], axis=0)
    for side, scr in enumerate(scrs):
        proj = nn_dot(w_ref[2 * C * side:2 * C * (side + 1)], aug)
        put_row(scr, row, SB, mask_f * sigmoid(proj[C:]) * proj[:C], 2 * half)
    return aug


def halves():
    return ((half, slice(WIDE * half, WIDE * (half + 1))) for half in range(2))


def pair_row(ref, row, ids_ref, half):
    return jnp.concatenate([ref[row, pl.ds(pl.multiple_of(ids_ref[8 * half + p], HALF), HALF), :] for p in range(8)], axis=0)


def normed_row(z_row, scale, offset):
    z_t = z_row.T.astype(F32)
    x_hat, inv_std = norm_rows(z_t)
    z_norm = (x_hat * scale + offset).astype(BF16)
    return x_hat, inv_std, z_norm


def pass_ids(ids_ref, tok_ref):
    for p in range(17):
        tok_ref[p] = ids_ref[p]


TOKEN = sds((17,), jnp.int32)
TOKEN_SPEC = pl.BlockSpec(memory_space=pltpu.SMEM)


def load_mask(m_ref, m_scr, t_scr, ids_ref):
    t_scr[...] = m_ref[...].astype(F32).T
    for half, cols in halves():
        m_scr[:, cols] = jnp.concatenate([t_scr[pl.ds(pl.multiple_of(ids_ref[8 * half + p], HALF), HALF), :] for p in range(8)], axis=0).T


def gated_kernel(half_id, ids_ref, z_ref, m_ref, w_ref, scale_ref, offset_ref, a_ref, b_ref, tok_ref, a_scr, b_scr, m_scr, t_scr):
    pass_ids(ids_ref, tok_ref)
    load_mask(m_ref, m_scr, t_scr, ids_ref)
    first = half_id * HALF + pl.program_id(0) * NB

    def body(row, carry):
        for half, cols in halves():
            _, _, z_norm = normed_row(pair_row(z_ref, row, ids_ref, half), scale_ref[...], offset_ref[...])
            gated_half(w_ref, (a_scr, b_scr), row, half, z_norm, m_scr[pl.ds(first + row, 1), cols])
        return carry

    lax.fori_loop(0, NB, body, 0, unroll=8)
    flush_rows(a_scr, a_ref)
    flush_rows(b_scr, b_ref)


def gated_call(half_id, ids, piece, mask_t, w_t, scale, offset):
    out_spec = pl.BlockSpec((C, NB, N), lambda r, ids: (0, r, 0))
    return pl.pallas_call(
        functools.partial(gated_kernel, half_id),
        grid_spec=pltpu.PrefetchScalarGridSpec(
            num_scalar_prefetch=1,
            grid=(HALF // NB,),
            in_specs=[
                pl.BlockSpec((NB, N, C), lambda r, ids: (r, 0, 0)),
                full_spec((NR, N)),
                full_spec((4 * C, C + 16)), full_spec((C, WIDE)), full_spec((C, WIDE)),
            ],
            out_specs=[out_spec, out_spec, TOKEN_SPEC],
            scratch_shapes=[pltpu.VMEM((4, C * SB, 128), F32)] * 2 + [pltpu.VMEM((NR, N), F32), pltpu.VMEM((N, NR), F32)],
        ),
        out_shape=[sds((C, HALF, N), BF16)] * 2 + [TOKEN],
        compiler_params=PARAMS,
        cost_estimate=COST,
        name="gated_rows",
    )(ids, piece, mask_t, w_t, scale, offset)


def lanes(val):
    half = val.shape[1] // 2
    return val[:, :half] + val[:, half:]


def own_kernel(ids_ref, z_ref, dy_ref, m_ref, w_ref, scale_ref, offset_ref, w_out_ref,
               a_ref, b_ref, dup_ref, don_ref, g1_ref, dbout_ref, dooff_ref, tok_ref, a_scr, b_scr, m_scr, t_scr):
    pass_ids(ids_ref, tok_ref)

    @pl.when(pl.program_id(0) == 0)
    def _():
        dbout_ref[...] = jnp.zeros_like(dbout_ref)
        dooff_ref[...] = jnp.zeros_like(dooff_ref)

    load_mask(m_ref, m_scr, t_scr, ids_ref)
    first = pl.program_id(0) * NB

    def body(row, carry):
        for half, cols in halves():
            _, _, z_norm = normed_row(pair_row(z_ref, row, ids_ref, half), scale_ref[...], offset_ref[...])
            aug = gated_half(w_ref, (a_scr, b_scr), row, half, z_norm, m_scr[pl.ds(first + row, 1), cols])
            sig_g = sigmoid(nn_dot(w_ref[4 * C:5 * C], aug))
            d_upd = sig_g * pair_row(dy_ref, row, ids_ref, half).T.astype(F32)
            g1_ref[row, :, cols] = d_upd * (1.0 - sig_g)
            d_upd16 = d_upd.astype(BF16)
            dup_ref[row, :, cols] = d_upd16
            d_onorm = nn_dot(w_out_ref[...], d_upd16).astype(BF16)
            don_ref[row, :, cols] = d_onorm
            dbout_ref[...] += lanes(d_upd16.astype(F32))
            dooff_ref[...] += lanes(d_onorm.astype(F32))
        return carry

    lax.fori_loop(0, NB, body, 0, unroll=4)
    flush_rows(a_scr, a_ref)
    flush_rows(b_scr, b_ref)


def own_call(ids, z_loc, dy_loc, m_loc, w_t, scale, offset, w_out):
    row_spec = pl.BlockSpec((NB, N, C), lambda r, ids: (r, 0, 0))
    t_spec = pl.BlockSpec((NB, C, N), lambda r, ids: (r, 0, 0))
    act_spec = pl.BlockSpec((C, NB, N), lambda r, ids: (0, r, 0))
    return pl.pallas_call(
        own_kernel,
        grid_spec=pltpu.PrefetchScalarGridSpec(
            num_scalar_prefetch=1,
            grid=(NQ,),
            in_specs=[row_spec, row_spec, full_spec((NR, N)),
                      full_spec((5 * C, C + 16)), full_spec((C, WIDE)), full_spec((C, WIDE)), full_spec((C, C))],
            out_specs=[act_spec, act_spec, t_spec, t_spec, t_spec, full_spec((C, 128)), full_spec((C, 128)), TOKEN_SPEC],
            scratch_shapes=[pltpu.VMEM((4, C * SB, 128), F32)] * 2 + [pltpu.VMEM((NR, N), F32), pltpu.VMEM((N, NR), F32)],
        ),
        out_shape=[sds((C, NR, N), BF16), sds((C, NR, N), BF16), sds((NR, C, N), BF16), sds((NR, C, N), BF16), sds((NR, C, N), F32), sds((C, 128), F32), sds((C, 128), F32), TOKEN],
        compiler_params=PARAMS,
        cost_estimate=COST,
        name="own_rows",
    )(ids, z_loc, dy_loc, m_loc, w_t, scale, offset, w_out)


CB = 32
CR = 32
CP = 64
FIRST = C // CB
LAST = FIRST + NR // CR


def out_kernel(ids_ref, a_ref, b_own0, b_own1, b_par0, b_par1, don_ref, dup_ref, g1_ref, w_out_ref, scale_ref, offset_ref,
               do_ref, dg_ref, *rest):
    dwout_ref, dosc_ref, dbg_ref, tok_ref, o_scr = rest[-5:]
    same0, same1, cross0, cross1 = rest[:-5] if len(rest) > 7 else [ref.at[h] for ref in rest[:2] for h in range(2)]
    step = pl.program_id(0)
    first_core = ids_ref[16] == 0

    @pl.when(step == 0)
    def _():
        pass_ids(ids_ref, tok_ref)
        dwout_ref[...] = jnp.zeros_like(dwout_ref)
        dosc_ref[...] = jnp.zeros_like(dosc_ref)
        dbg_ref[...] = jnp.zeros_like(dbg_ref)

    @pl.when(step < FIRST)
    def _():
        def prod(ch, carry):
            b_rows = jnp.concatenate([ref[ch] for ref in (b_own0, b_own1, b_par0, b_par1)], axis=0)
            val = nt_dot(a_ref[ch], b_rows)
            o_scr[0, pl.ds((step * CB + ch) * SO, NR), :] = jnp.where(first_core, val, pltpu.roll(val, 64, 1))
            return carry

        lax.fori_loop(0, CB, prod, 0, unroll=16)

    @pl.when((step >= FIRST) & (step < LAST))
    def _():
        def chain(row, carry):
            o_row = (step - FIRST) * CR + row
            o_hat, inv_std = norm_rows(get_row(o_scr, o_row, SO, (0,)))
            o_norm = (o_hat * scale_ref[...] + offset_ref[...]).astype(BF16)
            aug = jnp.concatenate([o_norm, ones_rows(C)], axis=0)
            upd = nn_dot(w_out_ref[...], aug).astype(BF16).astype(F32)
            d_gate = g1_ref[row] * upd
            dbg_ref[...] += d_gate
            dg_ref[row] = d_gate.astype(BF16)
            d_onorm = don_ref[row].astype(F32)
            dosc_ref[...] += d_onorm * o_hat
            grad_hat = d_onorm * scale_ref[...]
            mean_grad = jnp.mean(grad_hat, axis=0, keepdims=True)
            mean_proj = jnp.mean(grad_hat * o_hat, axis=0, keepdims=True)
            put_row(o_scr, o_row, SO, inv_std * (grad_hat - mean_grad - o_hat * mean_proj))
            dwout_ref[...] += nt_dot(o_norm, dup_ref[row])
            return carry

        lax.fori_loop(0, CR, chain, 0, unroll=8)

    @pl.when(step >= LAST)
    def _():
        lane = lax.broadcasted_iota(jnp.int32, (NB, C), 1)
        low = lane < 64
        even = lane % 64 < HALF

        def swap(left, right, keep, width):
            return jnp.where(keep, left, pltpu.roll(right, width, 1)), jnp.where(keep, pltpu.roll(left, C - width, 1), right)

        def pack(ch, carry):
            val = o_scr[0, pl.ds(((step - LAST) * CP + ch) * SO, NR), :]
            do_ref[ch] = jnp.where(first_core, val, pltpu.roll(val, 64, 1)).astype(BF16)
            g0, g1, g2, g3 = jnp.split(val, 4, axis=0)
            g0, g2 = swap(g0, g2, low, 64)
            g1, g3 = swap(g1, g3, low, 64)
            g0, g1 = swap(g0, g1, even, HALF)
            g2, g3 = swap(g2, g3, even, HALF)
            same0[ch] = jnp.where(first_core, g0, g2).astype(BF16)
            same1[ch] = jnp.where(first_core, g1, g3).astype(BF16)
            cross0[ch] = jnp.where(first_core, g2, g0).astype(BF16)
            cross1[ch] = jnp.where(first_core, g3, g1).astype(BF16)
            return carry

        lax.fori_loop(0, CP, pack, 0, unroll=8)


def piece_spec(width, blk):
    return pl.BlockSpec((width, HALF, N), lambda s, *ids: (s, blk, 0))


def prod_step(step):
    return jnp.minimum(step, FIRST - 1)


def chain_step(step):
    return jnp.clip(step - FIRST, 0, NR // CR - 1)


def pack_step(step):
    return jnp.clip(step - LAST, 0, C // CP - 1)


def out_call(chunk, ids, a_own, b_pieces, don, dup, g1, w_out_t, scale, offset):
    lane_spec = pl.BlockSpec((CR, C, C), lambda s, ids: (chain_step(s), 0, chunk))
    acc_spec = full_spec((C, C))
    if chunk % 2:
        packs, pack_spec = [sds((C, NB, C), BF16)] * 4, pl.BlockSpec((CP, NB, C), lambda s, ids: (pack_step(s), 0, 0))
    else:
        packs, pack_spec = [sds((2, C, NB, C), BF16)] * 2, pl.BlockSpec((2, CP, NB, C), lambda s, ids: (0, pack_step(s), 0, 0))
    b_specs = [pl.BlockSpec((CB, HALF, N), lambda s, ids, blk=blk: (prod_step(s), blk, 0)) for _, blk in b_pieces]
    return pl.pallas_call(
        out_kernel,
        grid_spec=pltpu.PrefetchScalarGridSpec(
            num_scalar_prefetch=1,
            grid=(LAST + C // CP,),
            in_specs=[pl.BlockSpec((CB, NR, N), lambda s, ids: (prod_step(s), 0, 0))] + b_specs
            + [lane_spec, lane_spec, lane_spec, full_spec((C, C + 16)), acc_spec, acc_spec],
            out_specs=[pl.BlockSpec((CP, NR, C), lambda s, ids: (pack_step(s), 0, 0)),
                       pl.BlockSpec((CR, C, C), lambda s, ids: (chain_step(s), 0, 0))] + [pack_spec] * len(packs) + [acc_spec] * 3 + [TOKEN_SPEC],
            scratch_shapes=[pltpu.VMEM((1, C * SO, C), F32)],
        ),
        out_shape=[sds((C, NR, C), BF16), sds((NR, C, C), BF16)] + packs + [sds((C, C), F32)] * 3 + [TOKEN],
        compiler_params=PARAMS,
        cost_estimate=COST,
        name="out_chain",
    )(ids, a_own, *(arr for arr, _ in b_pieces), don, dup, g1, w_out_t, scale, offset)


CK = 16


def da_kernel(count, *refs):
    do_refs, b_refs, da_ref = refs[:count], refs[count:5 * count], refs[-1]
    for ch in range(CK):
        do_row = jnp.concatenate([ref[ch] for ref in do_refs], axis=1)
        b_rows = jnp.concatenate([ref[ch] for ref in b_refs], axis=0)
        val = nn_dot(do_row, b_rows)
        for ref in refs[5 * count:-1]:
            val += ref[ch]
        da_ref[ch] = val.astype(da_ref.dtype)


def da_call(do_chunks, b_pieces, partial, dtype):
    row_spec = pl.BlockSpec((CK, NR, N), lambda s: (s, 0, 0))
    return pl.pallas_call(
        functools.partial(da_kernel, len(do_chunks)),
        grid=(C // CK,),
        in_specs=[pl.BlockSpec((CK, NR, C), lambda s: (s, 0, 0))] * len(do_chunks) + [piece_spec(CK, blk) for _, blk in b_pieces] + [row_spec] * len(partial),
        out_specs=row_spec,
        out_shape=sds((C, NR, N), dtype),
        compiler_params=PARAMS,
        cost_estimate=COST,
        name="grad_a",
    )(*do_chunks, *(arr for arr, _ in b_pieces), *partial)


def db_kernel(*refs):
    do_refs, a_refs, db_ref = refs[:16], refs[16:32], refs[32]
    for ch in range(CK):
        x_t = [jnp.concatenate([ref[ch] for ref in do_refs[8 * h:8 * h + 8]], axis=0).T for h in range(2)]
        total = None
        for g in range(4):
            lhs = jnp.concatenate([x[32 * g:32 * g + 32] for x in x_t], axis=0)
            half, sub = divmod(g, 2)
            rhs = jnp.concatenate([ref[ch, NB * sub:NB * (sub + 1), :] for ref in a_refs[8 * half:8 * half + 8]], axis=0)
            term = nn_dot(lhs, rhs)
            total = term if total is None else total + term
        db_ref[ch] = total.astype(BF16)


def do_spec(arr, half):
    if len(arr.shape) > 3:
        return pl.BlockSpec((None, CK, NB, C), lambda s: (half, s, 0, 0))
    return pl.BlockSpec((CK, NB, C), lambda s: (s, 0, 0))


def db_call(do_pieces, a_pieces):
    return pl.pallas_call(
        db_kernel,
        grid=(C // CK,),
        in_specs=[do_spec(*piece) for piece in do_pieces] + [piece_spec(CK, blk) for _, blk in a_pieces],
        out_specs=pl.BlockSpec((CK, NR, N), lambda s: (s, 0, 0)),
        out_shape=sds((C, NR, N), BF16),
        compiler_params=PARAMS,
        cost_estimate=COST,
        name="grad_b",
    )(*(arr for arr, _ in do_pieces), *(arr for arr, _ in a_pieces))


def in_kernel(ids_ref, z_ref, dy_ref, m_ref, da_ref, db_ref, dg0, dg1, dg2, dg3, w_ref, scale_ref, offset_ref, w_cat_ref,
              dz_ref, dw_ref, dbin_ref, dsc_ref, doff_ref, a_scr, b_scr, m_scr, t_scr):
    dgs = (dg0, dg1, dg2, dg3)

    @pl.when(pl.program_id(0) == 0)
    def _():
        dw_ref[...] = jnp.zeros_like(dw_ref)
        dbin_ref[...] = jnp.zeros_like(dbin_ref)
        dsc_ref[...] = jnp.zeros_like(dsc_ref)
        doff_ref[...] = jnp.zeros_like(doff_ref)

    def unpack(ch, carry):
        for src, scr in ((da_ref, a_scr), (db_ref, b_scr)):
            for lane in range(4):
                scr[lane, pl.ds(ch * SB, NB), :] = src[ch, :, C * lane:C * (lane + 1)].astype(F32)
        return carry

    lax.fori_loop(0, C, unpack, 0, unroll=4)

    load_mask(m_ref, m_scr, t_scr, ids_ref)
    first = pl.program_id(0) * NB

    def lanes4(val):
        return lanes(lanes(val))

    def body(row, carry):
        def full_row(ref):
            return jnp.concatenate([pair_row(ref, row, ids_ref, half) for half in range(2)], axis=0)

        x_hat, inv_std, z_norm = normed_row(full_row(z_ref), scale_ref[...], offset_ref[...])
        aug = jnp.concatenate([z_norm, ones_rows(N)], axis=0)
        mask_f = m_scr[pl.ds(first + row, 1), :]
        parts = []
        for side, scr in ((0, a_scr), (1, b_scr)):
            proj = nn_dot(w_ref[2 * C * side:2 * C * (side + 1)], aug)
            sig = sigmoid(proj[C:])
            d_proj = get_row(scr, row, SB, range(4)) * mask_f * sig
            d_lin = d_proj * proj[:C] * (1.0 - sig)
            dbin_ref[side] += lanes4(d_proj)
            dbin_ref[2 + side] += lanes4(d_lin)
            parts.append((d_proj.astype(BF16), d_lin.astype(BF16)))
        d_gate = jnp.concatenate([dg[row] for dg in dgs], axis=1)
        cat = jnp.concatenate([part[kind] for kind in range(2) for part in parts] + [d_gate], axis=0)
        dw_ref[...] += nt_dot(cat, z_norm)
        d_znorm = nn_dot(w_cat_ref[...], cat).astype(BF16).astype(F32)
        dsc_ref[...] += lanes4(d_znorm * x_hat)
        doff_ref[...] += lanes4(d_znorm)
        grad_hat = d_znorm * scale_ref[...]
        mean_grad = jnp.mean(grad_hat, axis=0, keepdims=True)
        mean_proj = jnp.mean(grad_hat * x_hat, axis=0, keepdims=True)
        d_zt = inv_std * (grad_hat - mean_grad - x_hat * mean_proj)
        d_row = (full_row(dy_ref).astype(F32) + d_zt.T).astype(BF16)
        for p in range(16):
            dz_ref[row, pl.ds(pl.multiple_of(ids_ref[p], HALF), HALF), :] = d_row[HALF * p:HALF * (p + 1)]
        return carry

    lax.fori_loop(0, NB, body, 0, unroll=8)


def in_call(ids, z_loc, dy_loc, m_loc, d_a, d_b, dg_chunks, w_t, scale, offset, w_cat):
    row_spec = pl.BlockSpec((NB, N, C), lambda r, ids: (r, 0, 0))
    act_spec = pl.BlockSpec((C, NB, N), lambda r, ids: (0, r, 0))
    return pl.pallas_call(
        in_kernel,
        grid_spec=pltpu.PrefetchScalarGridSpec(
            num_scalar_prefetch=1,
            grid=(NQ,),
            in_specs=[row_spec, row_spec, full_spec((NR, N)), act_spec, act_spec]
            + [pl.BlockSpec((NB, C, 128), lambda r, ids: (r, 0, 0))] * 4
            + [full_spec((4 * C, C + 16)), full_spec((C, N)), full_spec((C, N)), full_spec((C, 5 * C))],
            out_specs=[row_spec, full_spec((5 * C, C)), full_spec((4, C, C)), full_spec((C, 128)), full_spec((C, 128))],
            scratch_shapes=[pltpu.VMEM((4, C * SB, 128), F32)] * 2 + [pltpu.VMEM((NR, N), F32), pltpu.VMEM((N, NR), F32)],
        ),
        out_shape=[sds((NR, N, C), BF16), sds((5 * C, C), F32), sds((4, C, C), F32), sds((C, 128), F32), sds((C, 128), F32)],
        compiler_params=PARAMS,
        cost_estimate=COST,
        name="in_backward",
    )(ids, z_loc, dy_loc, m_loc, d_a, d_b, *dg_chunks, w_t, scale, offset, w_cat)


SHARD = 112
VECS = 6 * C
VEC_ROWS = (0, 1, 6, 7, 8, 9)


def sum_kernel(*refs):
    accs, acc_out, w_ref = refs[:7], refs[7], refs[8]
    total, src, recv, mine, send1, recv1, send2, recv2 = refs[9:]
    me = lax.axis_index('dap')

    def peer(step):
        return {'dap': lax.rem(me + step, 8)}

    barrier = pltpu.get_barrier_semaphore()
    for step in range(1, 8):
        pl.semaphore_signal(barrier, inc=1, device_id=peer(step), device_id_type=pl.DeviceIdType.MESH)
    for blk in range(5):
        src[C * blk:C * (blk + 1)] = w_ref[C * blk:C * (blk + 1)].T
    src[5 * C:VECS] = acc_out[...]
    rows = []
    for ref in accs:
        rows += [ref[n] for n in range(4)] if len(ref.shape) > 2 else [ref[...]]
    rows = [jnp.sum(val.T, axis=0, keepdims=True) for val in rows]
    src[VECS:] = jnp.concatenate(rows + [jnp.zeros((8 * SHARD - VECS - len(rows), C), F32)], axis=0)
    pl.semaphore_wait(barrier, 7)

    def shard(owner):
        return pl.ds(pl.multiple_of(owner * SHARD, 16), SHARD)

    copies = []
    for step in range(1, 8):
        copy = pltpu.make_async_remote_copy(
            src_ref=src.at[shard(lax.rem(me + step, 8))], dst_ref=recv.at[step], send_sem=send1.at[step], recv_sem=recv1.at[step],
            device_id=peer(step), device_id_type=pl.DeviceIdType.MESH)
        copy.start()
        copies.append(copy)
    val = src[shard(me), :]
    for step, copy in enumerate(copies):
        copy.wait()
        val += recv[step + 1]
    mine[...] = val.astype(BF16)
    total[shard(me), :] = val.astype(BF16)
    copies = []
    for step in range(1, 8):
        copy = pltpu.make_async_remote_copy(
            src_ref=mine, dst_ref=total.at[shard(me)], send_sem=send2.at[step], recv_sem=recv2.at[step],
            device_id=peer(step), device_id_type=pl.DeviceIdType.MESH)
        copy.start()
        copies.append(copy)
    for copy in copies:
        copy.wait()


def split_kernel(total, win_ref, wgate_ref, wout_ref, bin_ref, *vec_refs):
    for blk in range(4):
        win_ref[:, C * blk:C * (blk + 1)] = total[C * blk:C * (blk + 1)]
    wgate_ref[...] = total[4 * C:5 * C]
    wout_ref[...] = total[5 * C:VECS]
    vecs = total[VECS:VECS + 16]
    bin_ref[...] = vecs[2:6].reshape(4 * C)
    for ref, n in zip(vec_refs, VEC_ROWS):
        ref[...] = vecs[n:n + 1]


def vmem_specs(count):
    return [pl.BlockSpec(memory_space=pltpu.VMEM)] * count


def sum_call(*args):
    total = pl.pallas_call(
        sum_kernel,
        in_specs=vmem_specs(len(args)),
        out_specs=vmem_specs(1)[0],
        out_shape=sds((8 * SHARD, C), BF16),
        scratch_shapes=[pltpu.VMEM((8 * SHARD, C), F32), pltpu.VMEM((8, SHARD, C), F32), pltpu.VMEM((SHARD, C), BF16)]
        + [pltpu.SemaphoreType.DMA((8,))] * 4,
        compiler_params=pltpu.CompilerParams(collective_id=0, has_side_effects=True),
        cost_estimate=COST,
        name="sum_grads",
    )(*args)
    outs = [sds((C, width), BF16) for width in (4 * C, C, C)] + [sds((4 * C,), BF16)] + [sds((1, C), BF16)] * len(VEC_ROWS)
    return pl.pallas_call(
        split_kernel,
        in_specs=vmem_specs(1),
        out_specs=vmem_specs(len(outs)),
        out_shape=outs,
        cost_estimate=COST,
        name="split_grads",
    )(total)


def aug_weight(w_mat, bias):
    wide = jnp.zeros((w_mat.shape[1], 16), BF16).at[:, 0].set(bias)
    return jnp.concatenate([w_mat.T, wide], axis=1)


def column(vec, width):
    return jnp.broadcast_to(vec.astype(F32)[:, None], (C, width))


def local_grads(z_loc, mask_loc, dy_loc, ln_in_scale, ln_in_offset, w_in, b_in, ln_out_scale, ln_out_offset, w_out, b_out, w_gate, b_gate):
    me = lax.axis_index('dap')
    chip, core = me // 2, me % 2
    w_cat = jnp.concatenate([w_in, w_gate], axis=1)
    pa, pb, la, lb, gate = jnp.split(jnp.concatenate([w_cat, jnp.concatenate([b_in, b_gate])[None]], axis=0), 5, axis=1)
    w_t = jnp.concatenate([pa, la, pb, lb, gate], axis=1)
    w_t = aug_weight(w_t[:C], w_t[C])
    w_out_t = aug_weight(w_out, b_out)
    (in_scale, in_offset), wide_in = ((column(ln_in_scale, width), column(ln_in_offset, width)) for width in (WIDE, N))
    out_scale, out_offset = column(ln_out_scale, 128), column(ln_out_offset, 128)

    order = [((chip * 2) ^ HOPS[q][h]) * NR + core_of * NR + h * HALF for q in range(4) for core_of in range(2) for h in range(2)]
    ids = jnp.stack(order + [core]).astype(jnp.int32)
    mask_t = mask_loc.astype(BF16)

    def move(val, flips):
        return lax.ppermute(val, 'dap', [(d, d ^ flips) for d in range(8)])

    top, bottom = z_loc[:HALF], z_loc[HALF:]
    gathered = {}
    gathered[1, 0], gathered[1, 1] = move(top, HOPS[1][0]), move(bottom, HOPS[1][1])
    masks = {hop: move(mask_t, hop) for hop in (2, 4, 6)}
    gathered[2, 0], gathered[2, 1] = move(gathered[1, 0], HOPS[1][1]), move(gathered[1, 1], HOPS[1][0])
    gathered[3, 0], gathered[3, 1] = move(top, HOPS[3][0]), move(bottom, HOPS[3][1])

    a_own, b_own, dup, don, g1, acc_bout, acc_ooff, ids = own_call(ids, z_loc, dy_loc, mask_t, w_t, in_scale, in_offset, w_out)
    b_par, a_par = move(b_own, 1), move(a_own, 1)
    a_at = {(0, h, f): (val, h) for h in range(2) for f, val in ((0, a_own), (1, a_par))}
    b_at = {(0, h, f): (val, h) for h in range(2) for f, val in ((0, b_own), (1, b_par))}
    do_at, do_chunks, chunk_b, d_a, dg_chunks, sums = {}, [], [], [], [], []
    for q in range(4):
        for h in range(2):
            if q:
                act_a, act_b, ids = gated_call(h, ids, gathered[q, h], masks[HOPS[q][h]], w_t[:4 * C], in_scale, in_offset)
                a_at[q, h, 0], b_at[q, h, 0] = (act_a, 0), (act_b, 0)
                b_at[q, h, 1] = move(act_b, 1), 0
                a_at[q, h, 1] = move(act_a, 1), 0
        b_pieces = [b_at[q, h, f] for f in range(2) for h in range(2)]
        do_own, dg, *packs, acc_out, acc_osc, acc_bg, ids = out_call(q, ids, a_own, b_pieces, don, dup, g1, w_out_t, out_scale, out_offset)
        do_chunks.append(do_own)
        dg_chunks.append(dg)
        sums.append((acc_out, acc_osc, acc_bg))
        chunk_b += b_pieces
        if q:
            d_a = da_call(do_chunks, chunk_b, d_a, BF16 if q == 3 else F32)
            do_chunks, chunk_b, d_a = [], [], [d_a]
        for n, val in enumerate(packs):
            flip, h = divmod(n, 2) if q % 2 else (n, 0)
            flips = HOPS[q][h] ^ flip
            val = move(val, flips) if flips else val
            if q % 2:
                do_at[h, flips] = (val, h)
            else:
                do_at[0, flips], do_at[1, flips] = (val, 0), (val, 1)
    chunk_of = {(HOPS[q][h], h): q for q in range(4) for h in range(2)}
    d_b = db_call([do_at[h, s] for h in range(2) for s in range(8)],
                  [a_at[chunk_of[s & 6, h], h, s & 1] for h in range(2) for s in range(8)])
    d_z, acc_w, acc_bin, acc_isc, acc_ioff = in_call(ids, z_loc, dy_loc, mask_t, d_a[0], d_b, dg_chunks, w_t[:4 * C], *wide_in, w_cat)

    acc_out, acc_osc, acc_bg = (sum(parts[1:], parts[0]) for parts in zip(*sums))
    d_win, d_wgate, d_wout, *vecs = sum_call(acc_isc, acc_ioff, acc_bin, acc_osc, acc_ooff, acc_bout, acc_bg, acc_out, acc_w)
    d_bin, d_isc, d_ioff, d_osc, d_ooff, d_bout, d_bg = (vec.reshape(vec.size) for vec in vecs)
    return d_z, d_isc, d_ioff, d_win, d_bin, d_osc, d_ooff, d_wout, d_bout, d_wgate, d_bg


def solution(mesh):
    pair_spec = P(('batch', 'dap'), None, None)
    mask_spec = P(('batch', 'dap'), None)
    vec_rep = P(None)
    mat_rep = P(None, None)
    vec_part = P('batch')
    mat_part = P('batch', None)
    in_specs = (pair_spec, mask_spec, pair_spec, vec_rep, vec_rep, mat_rep, vec_rep, vec_rep, vec_rep, mat_rep, vec_rep, mat_rep, vec_rep)
    out_specs = (pair_spec, vec_part, vec_part, mat_part, vec_part, vec_part, vec_part, mat_part, vec_part, mat_part, vec_part)
    return jax.shard_map(local_grads, mesh=mesh, in_specs=in_specs, out_specs=out_specs, check_vma=False)
```
